32 devices in a mesh: rows: 8 (over z, x), probe: 4 (over y, core).
Axes of the slice: x: 2, y: 2, z: 4, core: 2. Of those that a mesh axis runs over, the one named last changes fastest.
Arguments:
- start_block: float32 [8, 32768], P('probe', 'rows'), may hold values from -6 to 6
- blocks: bfloat16 [1024, 128, 128], P('rows'), may hold values from 0 to 3, as said below
- block_rows: int32 [1024], P('rows'), may hold values from 0 to 31
- block_cols: int32 [1024], P('rows'), may hold values from 0 to 63
- counts: int32 [8], P('rows'), may hold values from 32 to 128, as said below
- boundary: int32 [2, 16384], P(None, 'rows'), may hold values from 0 to 4095, as said below
Outputs:
- basis: float32 [8, 32768], P('probe', 'rows')
- alpha_blocks: float32 [3, 8, 8], replicated
- beta_blocks: float32 [3, 8, 8], replicated
The draws below stay inside these ranges and needn't reach their ends.
Inputs may be any that keep to these rules, and one draw needn't show every extreme that they name: `blocks`: nonnegative edge weights, most entries zero. `counts`: one or more partitions have all 128 slots live. `boundary`: the 2048 entries of one list for one partition are distinct rows of that partition.
All inputs are finite; a program needn't handle non-finite values.
Results may differ from the reference program's by a relative error of at most 0.00525.
Values may be sent and summed in bfloat16 or wider, within the bound.
No kernel may reach another device: no remote copies, remote signals or barrier semaphores. Data moves between devices by JAX's collectives and lax.ppermute only.
A program may use at most 64 MiB of HBM per device.

```python
import jax
import jax.numpy as jnp
from jax import lax

PROBES = 8
BLOCK = 128
ROW_BLOCKS = 32
STEPS = 3
HALO = 2048
MAXB = 128
NODES = 32768
N_ROWS = 8


def draw_blocks(key, part):
    shape = (N_ROWS * MAXB, BLOCK, BLOCK)
    pick_key, value_key = jax.random.split(key)
    chance = jax.random.uniform(pick_key, shape, jnp.float32)
    weight = jnp.exp(jax.random.uniform(value_key, shape, jnp.float32, jnp.log(0.2), jnp.log(2.0)))
    return jnp.where(chance < 0.15, weight, 0.0).astype(jnp.bfloat16)


def draw_counts(key, part):
    first_key, second_key = jax.random.split(key)
    divisor = jax.random.randint(first_key, (N_ROWS,), 1, 5)
    live_slots = MAXB // divisor
    chosen = jax.random.randint(second_key, (), 0, N_ROWS)
    return jnp.where(jnp.arange(N_ROWS) == chosen, MAXB, live_slots).astype(jnp.int32)


def draw_boundary(key, part):
    keys_all = jax.random.split(key, 2 * N_ROWS)
    rows_dev = ROW_BLOCKS * BLOCK
    orders = jax.vmap(lambda one_key: jax.random.permutation(one_key, rows_dev))(keys_all)
    return orders[:, :HALO].reshape(2, N_ROWS * HALO).astype(jnp.int32)


def touch_ends(entries, own_key, smallest, top_value):
    longest = entries.shape.index(max(entries.shape))
    spots = []
    for shift in (0, 1):
        where = [jax.random.randint(jax.random.fold_in(own_key, axis), (), 0, length) for axis, length in enumerate(entries.shape)]
        where[longest] = (where[longest] + shift) % entries.shape[longest]
        spots.append(tuple(where))
    return entries.at[spots[0]].set(smallest).at[spots[1]].set(top_value)


def block_scale(rng, shape, pieces, low, high):
    factor_of = 1.0
    for position, parts in pieces:
        heights = jax.random.uniform(jax.random.fold_in(jax.random.fold_in(rng, 6), position), (parts,), jnp.float32, low / len(pieces), high / len(pieces))
        factor_of = factor_of * jnp.repeat(jnp.exp(heights), shape[position] // parts).reshape((-1,) + (1,) * (len(shape) - 1 - position))
    return factor_of


def normal_values(rng, dims, deviation, most, shards=(), held_as=jnp.bfloat16):
    array = deviation * jax.random.normal(rng, dims, jnp.float32)
    if shards:
        array = array * block_scale(rng, dims, shards, -0.22, 0.18)
    return jnp.clip(array, -most, most).astype(held_as)


def setup_inputs(seed: int = 0) -> dict:
    arg_keys = jax.random.split(jax.random.key(seed), 7)
    return {
        "start_block": normal_values(arg_keys[0], (PROBES, NODES), 1.0, 6.0, ((0, 4), (1, 8)), jnp.float32),
        "blocks": draw_blocks(jax.random.fold_in(arg_keys[6], 71), 0),
        "block_rows": touch_ends(jax.random.randint(arg_keys[2], (N_ROWS * MAXB,), 0, ROW_BLOCKS), jax.random.fold_in(arg_keys[2], 1), 0, ROW_BLOCKS - 1).astype(jnp.int32),
        "block_cols": touch_ends(jax.random.randint(arg_keys[3], (N_ROWS * MAXB,), 0, 2 * ROW_BLOCKS), jax.random.fold_in(arg_keys[3], 1), 0, (2 * ROW_BLOCKS) - 1).astype(jnp.int32),
        "counts": draw_counts(jax.random.fold_in(arg_keys[6], 71), 0),
        "boundary": draw_boundary(jax.random.fold_in(arg_keys[6], 71), 0),
    }


def apply_graph(scaled, blocks, block_rows, block_cols, counts, boundary):
    probe_count = scaled.shape[0]
    rows_dev = ROW_BLOCKS * BLOCK
    split_rows = scaled.reshape(probe_count, N_ROWS, rows_dev)
    bound = boundary.reshape(2, N_ROWS, HALO)
    from_lower = jnp.take_along_axis(jnp.roll(split_rows, 1, axis=1), jnp.roll(bound[1], 1, axis=0)[None], axis=2)
    from_upper = jnp.take_along_axis(jnp.roll(split_rows, -1, axis=1), jnp.roll(bound[0], -1, axis=0)[None], axis=2)
    extended = jnp.concatenate([split_rows, from_lower, from_upper], axis=2)
    extended = jnp.transpose(extended, (1, 0, 2))

    def partition(inputs):
        ext_part, tiles, tile_rows, tile_cols, live_count = inputs
        is_live = (jnp.arange(MAXB, dtype=jnp.int32) < live_count).astype(jnp.float32)
        tiles32 = tiles.astype(jnp.float32)
        columns = ext_part.reshape(probe_count, 2 * ROW_BLOCKS, BLOCK)
        x_cols = columns[:, tile_cols].astype(jnp.float32)
        x_rows = columns[:, :ROW_BLOCKS][:, tile_rows].astype(jnp.float32)
        forward = jnp.einsum('pkj,kij->pki', x_cols, tiles32) * is_live[None, :, None]
        backward = jnp.einsum('pki,kij->pkj', x_rows, tiles32) * is_live[None, :, None]
        row_sums = jnp.zeros((probe_count, ROW_BLOCKS, BLOCK), jnp.float32).at[:, tile_rows].add(forward)
        col_sums = jnp.zeros((probe_count, 2 * ROW_BLOCKS, BLOCK), jnp.float32).at[:, tile_cols].add(backward)
        summed = col_sums.reshape(probe_count, 2 * rows_dev)
        return summed.at[:, :rows_dev].add(row_sums.reshape(probe_count, rows_dev))
    summed = lax.map(partition, (extended, blocks.reshape(N_ROWS, MAXB, BLOCK, BLOCK), block_rows.reshape(N_ROWS, MAXB), block_cols.reshape(N_ROWS, MAXB), counts))
    own_part = summed[:, :, :rows_dev]
    lower_part = jnp.roll(summed[:, :, rows_dev:rows_dev + HALO], -1, axis=0)
    upper_part = jnp.roll(summed[:, :, rows_dev + HALO:], 1, axis=0)
    offsets = (jnp.arange(N_ROWS, dtype=jnp.int32) * rows_dev)[:, None]
    result = jnp.transpose(own_part, (1, 0, 2)).reshape(probe_count, NODES)
    result = result.at[:, (offsets + bound[1]).reshape(-1)].add(jnp.transpose(lower_part, (1, 0, 2)).reshape(probe_count, -1))
    result = result.at[:, (offsets + bound[0]).reshape(-1)].add(jnp.transpose(upper_part, (1, 0, 2)).reshape(probe_count, -1))
    return result

def gram_mean(left, right):
    return jnp.dot(left, right.T, precision=lax.Precision.HIGHEST) / NODES

def reference(start_block, blocks, block_rows, block_cols, counts, boundary):
    unit_rows = jnp.ones((1, NODES), jnp.bfloat16)
    degree = 1.0 + apply_graph(unit_rows, blocks, block_rows, block_cols, counts, boundary)[0]
    inv_root = 1.0 / jnp.sqrt(degree)

    def laplacian(vectors):
        scaled = (inv_root * vectors).astype(jnp.bfloat16)
        image = apply_graph(scaled, blocks, block_rows, block_cols, counts, boundary)
        return vectors - inv_root * (inv_root * vectors) - inv_root * image
    factor = jnp.linalg.cholesky(gram_mean(start_block, start_block))
    current = jax.scipy.linalg.solve_triangular(factor, start_block, lower=True)
    previous = jnp.zeros_like(current)
    coupling = jnp.zeros((PROBES, PROBES), jnp.float32)
    alpha_list = []
    beta_list = []
    for iteration in range(STEPS):
        image = laplacian(current)
        alpha_block = gram_mean(image, current)
        residual = image - jnp.dot(alpha_block, current, precision=lax.Precision.HIGHEST) - jnp.dot(coupling, previous, precision=lax.Precision.HIGHEST)
        factor = jnp.linalg.cholesky(gram_mean(residual, residual))
        previous = current
        current = jax.scipy.linalg.solve_triangular(factor, residual, lower=True)
        coupling = factor.T
        alpha_list.append(alpha_block)
        beta_list.append(factor)
    return (current, jnp.stack(alpha_list), jnp.stack(beta_list))
```

```python
import functools

import jax
import jax.numpy as jnp
from jax import lax
from jax.experimental import pallas as pl
from jax.experimental.pallas import tpu as pltpu
from jax.sharding import PartitionSpec as P

STEPS = 3
SHIFTS = (0.0, 1.0, 0.0)
UNROLL = 8
CHUNK = 16
F32 = jnp.float32
BF16 = jnp.bfloat16

SMEM = pl.BlockSpec(memory_space=pltpu.SMEM)
VMEM = pl.BlockSpec(memory_space=pltpu.VMEM)
ANY = pl.BlockSpec(memory_space=pl.ANY)


def dot(a, b, contract):
    return lax.dot_general(a, b, (contract, ((), ())), preferred_element_type=F32)


def exact_dot(a, b, contract):
    return lax.dot_general(
        a, b, (contract, ((), ())), precision=lax.Precision.HIGHEST, preferred_element_type=F32
    )


def tile_copy(blocks, tiles, sems, chunk):
    part = pl.ds(chunk * CHUNK, CHUNK)
    return pltpu.make_async_copy(blocks.at[part], tiles.at[part], sems.at[chunk])


def start_tiles(live, blocks, tiles, sems):
    for chunk in range(blocks.shape[0] // CHUNK):
        @pl.when(chunk * CHUNK < live)
        def _():
            tile_copy(blocks, tiles, sems, chunk).start()


def wait_tiles(live, blocks, tiles, sems):
    for chunk in range(blocks.shape[0] // CHUNK):
        @pl.when(chunk * CHUNK < live)
        def _():
            tile_copy(blocks, tiles, sems, chunk).wait()


def for_slots(slots, live, body):
    def group(index, carry):
        entries = []
        for lane in range(UNROLL):
            code = slots[index * UNROLL + lane]
            entries.append((code & 255, (code >> 8) & 255, code >> 16))
        body(entries)
        return carry

    lax.fori_loop(0, (live + UNROLL - 1) // UNROLL, group, 0)


def two_parts(values):
    high = values.astype(BF16).astype(F32)
    return jnp.concatenate([high, values - high], axis=0)


def add_products(entries, tiles, source, totals, forward):
    products = []
    for slot, row, col in entries:
        index = col if forward else row
        got = dot(source[index], tiles[slot], ((1,), (1,)) if forward else ((1,), (0,)))
        products.append(got[: got.shape[0] // 2] + got[got.shape[0] // 2 :])
    for (slot, row, col), got in zip(entries, products):
        index = row if forward else col
        totals[index] = totals[index] + got


def fill_one_hot(bound, table):
    width = table.shape[0]
    halo = bound.shape[1]
    for part in range(2):
        for begin in range(0, halo, width):
            low = bound[part : part + 1, begin : begin + width] & (width - 1)
            hit = lax.broadcasted_iota(jnp.int32, (width, width), 0) == low
            table[:, part * halo + begin : part * halo + begin + width] = jnp.where(
                hit, 1.0, 0.0
            ).astype(BF16)


def add_boundary(bound, table, spread, values):
    width = table.shape[0]
    shift = width.bit_length() - 1
    high_count = spread.shape[0] // 16
    high = jnp.concatenate([bound[0:1, :], bound[1:2, :]], axis=1) >> shift
    stacked = two_parts(values)
    for index in range(high_count):
        spread[16 * index : 16 * index + 16, :] = jnp.where(high == index, stacked, 0.0).astype(BF16)
    got = dot(spread[...], table[...], ((1,), (1,)))
    return [got[16 * i : 16 * i + 8] + got[16 * i + 8 : 16 * i + 16] for i in range(high_count)]


def pick_boundary(bound, table, source, out_low, out_up):
    width = table.shape[0]
    shift = width.bit_length() - 1
    halo = bound.shape[1]
    edge = source.shape[2]
    ratio = width // edge
    high_count = (source.shape[0] - 1) // ratio
    rows = jnp.concatenate(
        [
            jnp.concatenate([source[ratio * i + j] for j in range(ratio)], axis=1)
            for i in range(high_count)
        ],
        axis=0,
    )
    for part, out in enumerate((out_low, out_up)):
        for begin in range(0, halo, width):
            got = dot(rows, table[:, part * halo + begin : part * halo + begin + width], ((1,), (0,)))
            high = bound[part : part + 1, begin : begin + width] >> shift
            total = jnp.zeros((8, width), F32)
            for index in range(high_count):
                one = got[16 * index : 16 * index + 8] + got[16 * index + 8 : 16 * index + 16]
                total = total + jnp.where(high == index, one, 0.0)
            out[0:8, begin : begin + width] = total


def setup_kernel(counts, block_rows, block_cols, blocks, own, halo, sizes, low, up, tiles, sums, sems):
    live = counts[0]
    edge = blocks.shape[1]
    halo_blocks = low.shape[0]
    row_blocks = 2 * halo_blocks
    start_tiles(live, blocks, tiles, sems)
    sums[...] = jnp.zeros_like(sums)

    def place(slot, carry):
        own_count, halo_count = carry
        row = block_rows[slot]
        col = block_cols[slot]
        outside = (col >= row_blocks).astype(jnp.int32)
        code = slot | (row << 8) | ((col - row_blocks * outside) << 16)
        own[own_count] = code
        halo[halo_count] = code
        return own_count + 1 - outside, halo_count + outside

    own_count, halo_count = lax.fori_loop(0, live, place, (0, 0))
    empty = (row_blocks << 8) | (row_blocks << 16)
    for lane in range(UNROLL):
        own[own_count + lane] = empty
        halo[halo_count + lane] = empty
    sizes[0] = own_count
    sizes[1] = halo_count
    wait_tiles(live, blocks, tiles, sems)

    def add(entries):
        parts = [
            jnp.sum(tiles[slot].astype(F32).reshape(edge // 8, 8, edge), axis=0)
            for slot, row, col in entries
        ]
        for (slot, row, col), part in zip(entries, parts):
            sums[col] = sums[col] + part

    for_slots(halo, halo_count, add)
    for index in range(halo_blocks):
        low[index : index + 1, :] = jnp.sum(sums[index], axis=0, keepdims=True)
        up[index : index + 1, :] = jnp.sum(sums[halo_blocks + index], axis=0, keepdims=True)


def degree_kernel(counts, own, halo, sizes, blocks, degree, tiles, row_sums, col_sums, sems):
    live = counts[0]
    edge = blocks.shape[1]
    start_tiles(live, blocks, tiles, sems)
    row_sums[...] = jnp.zeros_like(row_sums)
    col_sums[...] = jnp.zeros_like(col_sums)
    ones = jnp.ones((16, edge), BF16)
    wait_tiles(live, blocks, tiles, sems)

    def add_rows(entries):
        parts = [dot(ones, tiles[slot], ((1,), (1,)))[0:8] for slot, row, col in entries]
        for (slot, row, col), part in zip(entries, parts):
            row_sums[row] = row_sums[row] + part

    def add_both(entries):
        parts = [
            jnp.sum(tiles[slot].astype(F32).reshape(edge // 8, 8, edge), axis=0)
            for slot, row, col in entries
        ]
        add_rows(entries)
        for (slot, row, col), part in zip(entries, parts):
            col_sums[col] = col_sums[col] + part

    for_slots(own, sizes[0], add_both)
    for_slots(halo, sizes[1], add_rows)
    for index in range(row_sums.shape[0] - 1):
        degree[:, index * edge : (index + 1) * edge] = (
            1.0 + row_sums[index] + jnp.sum(col_sums[index], axis=0, keepdims=True)
        )


def send_products(sizes, halo, tiles, bound, table, vector, scale, source, sums, out_low, out_up):
    edge = source.shape[2]
    row_blocks = source.shape[0] - 1
    half = row_blocks // 2
    for index in range(row_blocks):
        part = slice(index * edge, (index + 1) * edge)
        source[index] = two_parts(scale[:, part] * vector[:, part]).astype(BF16)
    source[row_blocks] = jnp.zeros_like(source[row_blocks])
    sums[...] = jnp.zeros_like(sums)
    for_slots(
        halo, sizes[1], lambda entries: add_products(entries, tiles, source, sums, False)
    )
    for index in range(half):
        part = slice(index * edge, (index + 1) * edge)
        out_low[8:16, part] = sums[index]
        out_up[8:16, part] = sums[half + index]
    pick_boundary(bound, table, source, out_low, out_up)


def first_kernel(
    counts, halo, sizes, place, blocks, bound, degree, got_low, got_up, *rest
):
    starts = rest[:-10]
    out_low, out_up, vector, scale, source, tiles, table, spread, sums, sems = rest[-10:]
    live = counts[0]
    edge = blocks.shape[1]
    start_tiles(live, blocks, tiles, sems)
    fill_one_hot(bound, table)
    each = starts[0].shape[0]
    for block in range(len(starts)):
        rows = starts[0][...]
        for other in range(1, len(starts)):
            rows = jnp.where(place[0] == (block ^ other), starts[other][...], rows)
        vector[block * each : (block + 1) * each, :] = rows
    received = jnp.concatenate(
        [got[i : i + 1, :] for got in (got_low, got_up) for i in range(got.shape[0])], axis=1
    )
    received = jnp.broadcast_to(received, (8, received.shape[1]))
    width = table.shape[0]
    for index, part in enumerate(add_boundary(bound, table, spread, received)):
        cols = slice(index * width, (index + 1) * width)
        total = degree[:, cols] + part
        root = lax.rsqrt(total)
        scale[:, cols] = root * (1.5 - 0.5 * total * root * root)
    wait_tiles(live, blocks, tiles, sems)
    send_products(sizes, halo, tiles, bound, table, vector, scale, source, sums, out_low, out_up)


def own_kernel(counts, own, sizes, blocks, source, image, tiles, sums, sems):
    live = counts[0]
    edge = blocks.shape[1]
    start_tiles(live, blocks, tiles, sems)
    sums[...] = jnp.zeros_like(sums)
    wait_tiles(live, blocks, tiles, sems)

    def add(entries):
        add_products(entries, tiles, source, sums, True)
        add_products(entries, tiles, source, sums, False)

    for_slots(own, sizes[0], add)
    for index in range(sums.shape[0] - 1):
        image[:, index * edge : (index + 1) * edge] = sums[index]


def next_vector(
    shift, live, halo, sizes, blocks, bound, previous, scale, image, got_low, got_up,
    vector, tiles, table, spread, sums, outside, sems,
):
    edge = blocks.shape[1]
    fill_one_hot(bound, table)
    halo_blocks = got_low.shape[1] // edge
    for index in range(halo_blocks):
        part = slice(index * edge, (index + 1) * edge)
        outside[index] = two_parts(got_low[0:8, part]).astype(BF16)
        outside[halo_blocks + index] = two_parts(got_up[0:8, part]).astype(BF16)
    outside[2 * halo_blocks] = jnp.zeros_like(outside[0])
    received = jnp.concatenate([got_low[8:16, :], got_up[8:16, :]], axis=1)
    added = add_boundary(bound, table, spread, received)
    width = table.shape[0]
    ratio = width // edge
    for index in range(sums.shape[0] - 1):
        part = slice((index % ratio) * edge, (index % ratio + 1) * edge)
        sums[index] = (
            added[index // ratio][:, part] + image[:, index * edge : (index + 1) * edge]
        )
    wait_tiles(live, blocks, tiles, sems)
    for_slots(
        halo, sizes[1], lambda entries: add_products(entries, tiles, outside, sums, True)
    )
    for index in range(sums.shape[0] - 1):
        part = slice(index * edge, (index + 1) * edge)
        old = previous[:, part]
        root = scale[:, part]
        vector[:, part] = root * (root * old) + root * sums[index] - shift * old


def middle_kernel(
    shift, counts, halo, sizes, blocks, bound, previous, scale, image, got_low, got_up,
    out_low, out_up, vector, source, tiles, table, spread, sums, outside, sems,
):
    live = counts[0]
    start_tiles(live, blocks, tiles, sems)
    next_vector(
        shift, live, halo, sizes, blocks, bound, previous, scale, image, got_low, got_up,
        vector, tiles, table, spread, sums, outside, sems,
    )
    send_products(sizes, halo, tiles, bound, table, vector, scale, source, sums, out_low, out_up)


def three_parts(values):
    high = values.astype(BF16)
    rest = values - high.astype(F32)
    middle = rest.astype(BF16)
    return [high, middle, (rest - middle.astype(F32)).astype(BF16)]


def last_kernel(
    shift, counts, halo, sizes, blocks, bound, scale, image, got_low, got_up, *rest
):
    vectors = rest[:STEPS]
    gram, vector, tiles, table, spread, sums, outside, sems = rest[STEPS:]
    live = counts[0]
    start_tiles(live, blocks, tiles, sems)
    next_vector(
        shift, live, halo, sizes, blocks, bound, vectors[-1], scale, image, got_low, got_up,
        vector, tiles, table, spread, sums, outside, sems,
    )
    basis = jnp.concatenate([one[...] for one in vectors] + [vector[...]], axis=0)
    size = basis.shape[0]
    parts = jnp.concatenate(three_parts(basis), axis=0)
    wide = dot(parts, parts, ((1,), (1,)))
    total = sum(
        wide[i * size : (i + 1) * size, j * size : (j + 1) * size]
        for i in reversed(range(3))
        for j in reversed(range(3))
    )
    packed = jnp.concatenate([total[8 * i : 8 * i + 8, :] for i in range(size // 8)], axis=1)
    for copy in range(gram.shape[0] // 8):
        gram[8 * copy : 8 * copy + 8, :] = packed


def final_kernel(node_total, place, grams, *rest):
    vectors = rest[: STEPS + 1]
    basis, alphas, betas = rest[STEPS + 1 :]
    size = 8 * (STEPS + 1)
    packed = grams[0:8, :]
    for copy in range(1, grams.shape[0] // 8):
        packed = packed + grams[8 * copy : 8 * copy + 8, :]
    packed = packed * (1.0 / node_total)
    gram = jnp.concatenate(
        [packed[:, i * size : (i + 1) * size] for i in range(STEPS + 1)], axis=0
    )
    row_ids = lax.broadcasted_iota(jnp.int32, (size, size), 0)
    col_ids = lax.broadcasted_iota(jnp.int32, (size, size), 1)
    unit = jnp.where(row_ids == col_ids, 1.0, 0.0)
    work = jnp.concatenate([gram, unit], axis=1)
    rows = lax.broadcasted_iota(jnp.int32, (size, 2 * size), 0)
    pivots = jnp.ones((size, 2 * size), F32)
    for k in range(size):
        pivot = jnp.broadcast_to(work[k : k + 1, k : k + 1], (1, 2 * size))
        line = work[k : k + 1, :]
        factor = jnp.broadcast_to(work[:, k : k + 1], (size, 2 * size))
        pivots = jnp.where(rows == k, pivot, pivots)
        work = work - jnp.where(rows > k, factor * (line / pivot), 0.0)
    work = work / jnp.sqrt(pivots)
    upper = jnp.where(row_ids <= col_ids, work[:, :size], 0.0)
    inverse = work[:, size:]
    own = jnp.where(row_ids // 8 == col_ids // 8, inverse, 0.0)
    moved = jnp.concatenate(
        [jnp.zeros((8, size), F32)]
        + [
            jnp.concatenate(
                [jnp.zeros((8, 8), F32), own[8 * i : 8 * i + 8, : size - 8]], axis=1
            )
            for i in range(STEPS)
        ],
        axis=0,
    )
    by_last = exact_dot(moved, upper, ((1,), (1,)))
    by_own = exact_dot(own, upper, ((1,), (1,)))
    small = unit[0:8, 0:8]

    def piece(table, i, j):
        return table[8 * i : 8 * i + 8, 8 * j : 8 * j + 8]

    for j in range(STEPS):
        beta = piece(by_last, j + 1, j + 1)
        alpha = (1.0 - SHIFTS[j]) * small - piece(by_last, j + 1, j)
        if j:
            alpha = alpha + exact_dot(piece(by_own, j, j - 1), piece(by_last, j, j), ((1,), (0,)))
        betas[j] = jnp.where(row_ids[0:8, 0:8] >= col_ids[0:8, 0:8], beta, 0.0)
        alphas[j] = alpha
    last = inverse[size - 8 :, :] * (-1.0) ** STEPS
    each = basis.shape[0]
    ids = lax.broadcasted_iota(jnp.int32, (8, size), 0)
    chosen = jnp.zeros((8, size), F32)
    for index in range(each):
        line = jnp.sum(jnp.where(ids == place[0] * each + index, last, 0.0), axis=0, keepdims=True)
        chosen = jnp.where(ids == index, line, chosen)
    total = exact_dot(chosen, jnp.concatenate([one[...] for one in vectors], axis=0), ((1,), (0,)))
    basis[...] = total[0:each]


def local(start_block, blocks, block_rows, block_cols, counts, boundary):
    each, rows_dev = start_block.shape
    slot_count, edge, _ = blocks.shape
    halo_width = boundary.shape[1]
    parts = lax.axis_size("rows")
    groups = lax.axis_size("probe")
    node_total = rows_dev * parts
    row_blocks = rows_dev // edge
    halo_blocks = halo_width // edge
    probes = each * groups
    width = 2 * edge
    shape = jax.ShapeDtypeStruct
    place = lax.axis_index("probe").astype(jnp.int32).reshape(1)

    forward = [(i, (i + 1) % parts) for i in range(parts)]
    backward = [(target, source) for source, target in forward]

    def exchange(to_low, to_up):
        from_up = lax.ppermute(to_low, "rows", backward)
        from_low = lax.ppermute(to_up, "rows", forward)
        return from_low, from_up

    tile_scratch = pltpu.VMEM(blocks.shape, BF16)
    sems = pltpu.SemaphoreType.DMA((slot_count // CHUNK,))
    sums = pltpu.VMEM((row_blocks + 1, 8, edge), F32)
    table = pltpu.VMEM((width, 2 * halo_width), BF16)
    spread = pltpu.VMEM((16 * (rows_dev // width), 2 * halo_width), BF16)
    source_shape = (row_blocks + 1, 16, edge)

    def call(body, in_specs, out_shape, out_specs, scratch, name):
        return pl.pallas_call(
            body,
            out_shape=out_shape,
            in_specs=in_specs,
            out_specs=out_specs,
            scratch_shapes=scratch,
            name=name,
            compiler_params=pltpu.CompilerParams(vmem_limit_bytes=40 << 20),
        )

    starts = [start_block]
    for other in range(1, groups):
        pairs = [(i, i ^ other) for i in range(groups)]
        starts.append(lax.ppermute(start_block, "probe", pairs))

    own, halo, sizes, low, up = call(
        setup_kernel,
        [SMEM, SMEM, SMEM, ANY],
        (
            shape((slot_count + UNROLL,), jnp.int32),
            shape((slot_count + UNROLL,), jnp.int32),
            shape((2,), jnp.int32),
            shape((halo_blocks, edge), F32),
            shape((halo_blocks, edge), F32),
        ),
        (SMEM, SMEM, SMEM, VMEM, VMEM),
        [tile_scratch, sums, sems],
        "setup",
    )(counts, block_rows, block_cols, blocks)
    got_low, got_up = exchange(low, up)
    degree = call(
        degree_kernel,
        [SMEM, SMEM, SMEM, SMEM, ANY],
        shape((8, rows_dev), F32),
        VMEM,
        [tile_scratch, sums, sums, sems],
        "degree",
    )(counts, own, halo, sizes, blocks)

    message = shape((16, halo_width), F32)
    vector_shape = shape((probes, rows_dev), F32)
    to_low, to_up, vector, scale, source = call(
        first_kernel,
        [SMEM, SMEM, SMEM, SMEM, ANY] + [VMEM] * (4 + groups),
        (message, message, vector_shape, vector_shape, shape(source_shape, BF16)),
        (VMEM,) * 5,
        [tile_scratch, table, spread, sums, sems],
        "first",
    )(counts, halo, sizes, place, blocks, boundary, degree, got_low, got_up, *starts)

    vectors = [vector]
    for step in range(STEPS):
        got_low, got_up = exchange(to_low, to_up)
        image = call(
            own_kernel,
            [SMEM, SMEM, SMEM, ANY, VMEM],
            vector_shape,
            VMEM,
            [tile_scratch, sums, sems],
            f"own{step}",
        )(counts, own, sizes, blocks, source)
        scratch = [
            tile_scratch, table, spread, sums, pltpu.VMEM((2 * halo_blocks + 1, 16, edge), BF16), sems,
        ]
        if step + 1 < STEPS:
            to_low, to_up, vector, source = call(
                functools.partial(middle_kernel, SHIFTS[step]),
                [SMEM, SMEM, SMEM, ANY] + [VMEM] * 6,
                (message, message, vector_shape, shape(source_shape, BF16)),
                (VMEM,) * 4,
                scratch,
                f"middle{step}",
            )(counts, halo, sizes, blocks, boundary, vectors[-1], scale, image, got_low, got_up)
        else:
            grams, vector = call(
                functools.partial(last_kernel, SHIFTS[step]),
                [SMEM, SMEM, SMEM, ANY] + [VMEM] * (5 + STEPS),
                (shape((8 * parts, 128), F32), vector_shape),
                (VMEM,) * 2,
                scratch,
                "last",
            )(counts, halo, sizes, blocks, boundary, scale, image, got_low, got_up, *vectors)
        vectors.append(vector)
    gathered = lax.all_to_all(grams, "rows", 0, 0, tiled=True)
    return call(
        functools.partial(final_kernel, float(node_total)),
        [SMEM] + [VMEM] * (2 + STEPS),
        (
            shape((each, rows_dev), F32),
            shape((STEPS, probes, probes), F32),
            shape((STEPS, probes, probes), F32),
        ),
        (VMEM,) * 3,
        [],
        "final",
    )(place, gathered, *vectors)


def solution(mesh):
    in_specs = (
        P("probe", "rows"),
        P("rows", None, None),
        P("rows"),
        P("rows"),
        P("rows"),
        P(None, "rows"),
    )
    out_specs = (P("probe", "rows"), P(), P())
    return jax.shard_map(local, mesh=mesh, in_specs=in_specs, out_specs=out_specs, check_vma=False)
```

```python
import functools

import jax
import jax.numpy as jnp
from jax import lax
from jax.experimental import pallas as pl
from jax.experimental.pallas import tpu as pltpu
from jax.sharding import PartitionSpec as P

STEPS = 3
SHIFTS = (0.0, 1.0, 0.0)
UNROLL = 8
LIMIT = 16 << 20
F32 = jnp.float32
BF16 = jnp.bfloat16

SMEM = pl.BlockSpec(memory_space=pltpu.SMEM)
VMEM = pl.BlockSpec(memory_space=pltpu.VMEM)
ANY = pl.BlockSpec(memory_space=pl.ANY)


def dot(a, b, contract):
    return lax.dot_general(a, b, (contract, ((), ())), preferred_element_type=F32)


def exact_dot(a, b, contract):
    return lax.dot_general(
        a, b, (contract, ((), ())), precision=lax.Precision.HIGHEST, preferred_element_type=F32
    )


def for_slots(slots, live, body):
    def group(index, carry):
        entries = []
        for lane in range(UNROLL):
            code = slots[index * UNROLL + lane]
            entries.append((code & 255, (code >> 8) & 255, code >> 16))
        body(entries)
        return carry

    lax.fori_loop(0, (live + UNROLL - 1) // UNROLL, group, 0)


def two_parts(values):
    high = values.astype(BF16).astype(F32)
    return jnp.concatenate([high, values - high], axis=0)


def add_products(entries, tiles, source, totals, forward):
    products = []
    for slot, row, col in entries:
        index = col if forward else row
        got = dot(source[index], tiles[slot], ((1,), (1,)) if forward else ((1,), (0,)))
        products.append(got[: got.shape[0] // 2] + got[got.shape[0] // 2 :])
    for (slot, row, col), got in zip(entries, products):
        index = row if forward else col
        totals[index] = totals[index] + got


def fill_one_hot(bound, table):
    width = table.shape[0]
    halo = bound.shape[1]
    for part in range(2):
        for begin in range(0, halo, width):
            low = bound[part : part + 1, begin : begin + width] & (width - 1)
            hit = lax.broadcasted_iota(jnp.int32, (width, width), 0) == low
            table[:, part * halo + begin : part * halo + begin + width] = jnp.where(
                hit, 1.0, 0.0
            ).astype(BF16)


def add_boundary(bound, table, spread, values):
    width = table.shape[0]
    shift = width.bit_length() - 1
    high_count = spread.shape[0] // 16
    high = jnp.concatenate([bound[0:1, :], bound[1:2, :]], axis=1) >> shift
    stacked = two_parts(values)
    for index in range(high_count):
        spread[16 * index : 16 * index + 16, :] = jnp.where(high == index, stacked, 0.0).astype(BF16)
    got = dot(spread[...], table[...], ((1,), (1,)))
    return [got[16 * i : 16 * i + 8] + got[16 * i + 8 : 16 * i + 16] for i in range(high_count)]


def pick_boundary(bound, table, source, out_low, out_up):
    width = table.shape[0]
    shift = width.bit_length() - 1
    halo = bound.shape[1]
    edge = source.shape[2]
    ratio = width // edge
    high_count = (source.shape[0] - 1) // ratio
    rows = jnp.concatenate(
        [
            jnp.concatenate([source[ratio * i + j] for j in range(ratio)], axis=1)
            for i in range(high_count)
        ],
        axis=0,
    )
    for part, out in enumerate((out_low, out_up)):
        for begin in range(0, halo, width):
            got = dot(rows, table[:, part * halo + begin : part * halo + begin + width], ((1,), (0,)))
            high = bound[part : part + 1, begin : begin + width] >> shift
            total = jnp.zeros((8, width), F32)
            for index in range(high_count):
                one = got[16 * index : 16 * index + 8] + got[16 * index + 8 : 16 * index + 16]
                total = total + jnp.where(high == index, one, 0.0)
            out[0:8, begin : begin + width] = total


def list_kernel(
    row_blocks, counts_in, rows_in, cols_in, own, halo, sizes, counts, block_rows, block_cols, sems
):
    pairs = ((counts_in, counts), (rows_in, block_rows), (cols_in, block_cols))
    copies = [
        pltpu.make_async_copy(source, target, sems.at[index])
        for index, (source, target) in enumerate(pairs)
    ]
    for copy in copies:
        copy.start()
    for copy in copies:
        copy.wait()

    def place(slot, carry):
        own_count, halo_count = carry
        row = block_rows[slot]
        col = block_cols[slot]
        outside = (col >= row_blocks).astype(jnp.int32)
        code = slot | (row << 8) | ((col - row_blocks * outside) << 16)
        own[own_count] = code
        halo[halo_count] = code
        return own_count + 1 - outside, halo_count + outside

    own_count, halo_count = lax.fori_loop(0, counts[0], place, (0, 0))
    empty = (row_blocks << 8) | (row_blocks << 16)
    for lane in range(UNROLL):
        own[own_count + lane] = empty
        halo[halo_count + lane] = empty
    sizes[0] = own_count
    sizes[1] = halo_count


def setup_kernel(halo, sizes, tiles, low, up, sums):
    edge = tiles.shape[1]
    halo_blocks = low.shape[0]
    sums[...] = jnp.zeros_like(sums)

    def add(entries):
        parts = [
            jnp.sum(tiles[slot].astype(F32).reshape(edge // 8, 8, edge), axis=0)
            for slot, row, col in entries
        ]
        for (slot, row, col), part in zip(entries, parts):
            sums[col] = sums[col] + part

    for_slots(halo, sizes[1], add)
    for index in range(halo_blocks):
        low[index : index + 1, :] = jnp.sum(sums[index], axis=0, keepdims=True)
        up[index : index + 1, :] = jnp.sum(sums[halo_blocks + index], axis=0, keepdims=True)


def degree_kernel(own, halo, sizes, tiles, bound, degree, table, row_sums, col_sums):
    edge = tiles.shape[1]
    fill_one_hot(bound, table)
    row_sums[...] = jnp.zeros_like(row_sums)
    col_sums[...] = jnp.zeros_like(col_sums)
    ones = jnp.ones((16, edge), BF16)

    def add_rows(entries):
        parts = [dot(ones, tiles[slot], ((1,), (1,)))[0:8] for slot, row, col in entries]
        for (slot, row, col), part in zip(entries, parts):
            row_sums[row] = row_sums[row] + part

    def add_both(entries):
        parts = [
            jnp.sum(tiles[slot].astype(F32).reshape(edge // 8, 8, edge), axis=0)
            for slot, row, col in entries
        ]
        add_rows(entries)
        for (slot, row, col), part in zip(entries, parts):
            col_sums[col] = col_sums[col] + part

    for_slots(own, sizes[0], add_both)
    for_slots(halo, sizes[1], add_rows)
    for index in range(row_sums.shape[0] - 1):
        degree[:, index * edge : (index + 1) * edge] = (
            1.0 + row_sums[index] + jnp.sum(col_sums[index], axis=0, keepdims=True)
        )


def send_products(sizes, halo, tiles, bound, table, vector, scale, source, sums, out_low, out_up):
    edge = source.shape[2]
    row_blocks = source.shape[0] - 1
    half = row_blocks // 2
    for index in range(row_blocks):
        part = slice(index * edge, (index + 1) * edge)
        source[index] = two_parts(scale[:, part] * vector[:, part]).astype(BF16)
    source[row_blocks] = jnp.zeros_like(source[row_blocks])
    sums[...] = jnp.zeros_like(sums)
    for_slots(
        halo, sizes[1], lambda entries: add_products(entries, tiles, source, sums, False)
    )
    for index in range(half):
        part = slice(index * edge, (index + 1) * edge)
        out_low[8:16, part] = sums[index]
        out_up[8:16, part] = sums[half + index]
    pick_boundary(bound, table, source, out_low, out_up)


def first_kernel(
    halo, sizes, tiles, bound, table, degree, got_low, got_up, *rest
):
    starts = rest[:-7]
    out_low, out_up, vector, scale, source, spread, sums = rest[-7:]
    each = starts[0].shape[0]
    place = lax.axis_index("probe")
    for block in range(len(starts)):
        rows = starts[0][...]
        for other in range(1, len(starts)):
            rows = jnp.where(place == (block ^ other), starts[other][...], rows)
        vector[block * each : (block + 1) * each, :] = rows
    received = jnp.concatenate(
        [got[i : i + 1, :] for got in (got_low, got_up) for i in range(got.shape[0])], axis=1
    )
    received = jnp.broadcast_to(received, (8, received.shape[1]))
    width = table.shape[0]
    for index, part in enumerate(add_boundary(bound, table, spread, received)):
        cols = slice(index * width, (index + 1) * width)
        total = degree[:, cols] + part
        root = lax.rsqrt(total)
        scale[:, cols] = root * (1.5 - 0.5 * total * root * root)
    send_products(sizes, halo, tiles, bound, table, vector, scale, source, sums, out_low, out_up)


def own_kernel(own, sizes, tiles, source, image, sums):
    edge = tiles.shape[1]
    sums[...] = jnp.zeros_like(sums)

    def add(entries):
        add_products(entries, tiles, source, sums, True)
        add_products(entries, tiles, source, sums, False)

    for_slots(own, sizes[0], add)
    for index in range(sums.shape[0] - 1):
        image[:, index * edge : (index + 1) * edge] = sums[index]


def next_vector(
    shift, halo, sizes, tiles, bound, table, previous, scale, image, got_low, got_up,
    vector, spread, sums, outside,
):
    edge = tiles.shape[1]
    halo_blocks = got_low.shape[1] // edge
    for index in range(halo_blocks):
        part = slice(index * edge, (index + 1) * edge)
        outside[index] = two_parts(got_low[0:8, part]).astype(BF16)
        outside[halo_blocks + index] = two_parts(got_up[0:8, part]).astype(BF16)
    outside[2 * halo_blocks] = jnp.zeros_like(outside[0])
    received = jnp.concatenate([got_low[8:16, :], got_up[8:16, :]], axis=1)
    added = add_boundary(bound, table, spread, received)
    width = table.shape[0]
    ratio = width // edge
    for index in range(sums.shape[0] - 1):
        part = slice((index % ratio) * edge, (index % ratio + 1) * edge)
        sums[index] = (
            added[index // ratio][:, part] + image[:, index * edge : (index + 1) * edge]
        )
    for_slots(
        halo, sizes[1], lambda entries: add_products(entries, tiles, outside, sums, True)
    )
    for index in range(sums.shape[0] - 1):
        part = slice(index * edge, (index + 1) * edge)
        old = previous[:, part]
        root = scale[:, part]
        vector[:, part] = root * (root * old) + root * sums[index] - shift * old


def middle_kernel(
    shift, halo, sizes, tiles, bound, table, previous, scale, image, got_low, got_up,
    out_low, out_up, vector, source, spread, sums, outside,
):
    next_vector(
        shift, halo, sizes, tiles, bound, table, previous, scale, image, got_low, got_up,
        vector, spread, sums, outside,
    )
    send_products(sizes, halo, tiles, bound, table, vector, scale, source, sums, out_low, out_up)


def three_parts(values):
    high = values.astype(BF16)
    rest = values - high.astype(F32)
    middle = rest.astype(BF16)
    return [high, middle, (rest - middle.astype(F32)).astype(BF16)]


def last_kernel(
    shift, halo, sizes, tiles, bound, table, scale, image, got_low, got_up, *rest
):
    vectors = rest[:STEPS]
    gram, vector, spread, sums, outside = rest[STEPS:]
    next_vector(
        shift, halo, sizes, tiles, bound, table, vectors[-1], scale, image, got_low, got_up,
        vector, spread, sums, outside,
    )
    basis = jnp.concatenate([one[...] for one in vectors] + [vector[...]], axis=0)
    size = basis.shape[0]
    parts = jnp.concatenate(three_parts(basis), axis=0)
    wide = dot(parts, parts, ((1,), (1,)))
    total = sum(
        wide[i * size : (i + 1) * size, j * size : (j + 1) * size]
        for i in reversed(range(3))
        for j in reversed(range(3))
    )
    packed = jnp.concatenate([total[8 * i : 8 * i + 8, :] for i in range(size // 8)], axis=1)
    for copy in range(gram.shape[0] // 8):
        gram[8 * copy : 8 * copy + 8, :] = packed


def final_kernel(node_total, grams, *rest):
    vectors = rest[: STEPS + 1]
    basis, alphas, betas = rest[STEPS + 1 :]
    size = 8 * (STEPS + 1)
    packed = grams[0:8, :]
    for copy in range(1, grams.shape[0] // 8):
        packed = packed + grams[8 * copy : 8 * copy + 8, :]
    packed = packed * (1.0 / node_total)
    gram = jnp.concatenate(
        [packed[:, i * size : (i + 1) * size] for i in range(STEPS + 1)], axis=0
    )
    row_ids = lax.broadcasted_iota(jnp.int32, (size, size), 0)
    col_ids = lax.broadcasted_iota(jnp.int32, (size, size), 1)
    unit = jnp.where(row_ids == col_ids, 1.0, 0.0)
    work = jnp.concatenate([gram, unit], axis=1)
    rows = lax.broadcasted_iota(jnp.int32, (size, 2 * size), 0)
    pivots = jnp.ones((size, 2 * size), F32)
    for k in range(size):
        pivot = jnp.broadcast_to(work[k : k + 1, k : k + 1], (1, 2 * size))
        line = work[k : k + 1, :]
        factor = jnp.broadcast_to(work[:, k : k + 1], (size, 2 * size))
        pivots = jnp.where(rows == k, pivot, pivots)
        work = work - jnp.where(rows > k, factor * (line / pivot), 0.0)
    work = work / jnp.sqrt(pivots)
    upper = jnp.where(row_ids <= col_ids, work[:, :size], 0.0)
    inverse = work[:, size:]
    own = jnp.where(row_ids // 8 == col_ids // 8, inverse, 0.0)
    moved = jnp.concatenate(
        [jnp.zeros((8, size), F32)]
        + [
            jnp.concatenate(
                [jnp.zeros((8, 8), F32), own[8 * i : 8 * i + 8, : size - 8]], axis=1
            )
            for i in range(STEPS)
        ],
        axis=0,
    )
    by_last = exact_dot(moved, upper, ((1,), (1,)))
    by_own = exact_dot(own, upper, ((1,), (1,)))
    small = unit[0:8, 0:8]

    def piece(table, i, j):
        return table[8 * i : 8 * i + 8, 8 * j : 8 * j + 8]

    for j in range(STEPS):
        beta = piece(by_last, j + 1, j + 1)
        alpha = (1.0 - SHIFTS[j]) * small - piece(by_last, j + 1, j)
        if j:
            alpha = alpha + exact_dot(piece(by_own, j, j - 1), piece(by_last, j, j), ((1,), (0,)))
        betas[j] = jnp.where(row_ids[0:8, 0:8] >= col_ids[0:8, 0:8], beta, 0.0)
        alphas[j] = alpha
    last = inverse[size - 8 :, :] * (-1.0) ** STEPS
    each = basis.shape[0]
    place = lax.axis_index("probe")
    ids = lax.broadcasted_iota(jnp.int32, (8, size), 0)
    chosen = jnp.zeros((8, size), F32)
    for index in range(each):
        line = jnp.sum(jnp.where(ids == place * each + index, last, 0.0), axis=0, keepdims=True)
        chosen = jnp.where(ids == index, line, chosen)
    total = exact_dot(chosen, jnp.concatenate([one[...] for one in vectors], axis=0), ((1,), (0,)))
    basis[...] = total[0:each]


def local(start_block, blocks, block_rows, block_cols, counts, boundary):
    each, rows_dev = start_block.shape
    slot_count, edge, _ = blocks.shape
    halo_width = boundary.shape[1]
    parts = lax.axis_size("rows")
    groups = lax.axis_size("probe")
    node_total = rows_dev * parts
    row_blocks = rows_dev // edge
    halo_blocks = halo_width // edge
    probes = each * groups
    width = 2 * edge
    shape = jax.ShapeDtypeStruct

    forward = [(i, (i + 1) % parts) for i in range(parts)]
    backward = [(target, source) for source, target in forward]

    def exchange(to_low, to_up):
        from_up = lax.ppermute(to_low, "rows", backward)
        from_low = lax.ppermute(to_up, "rows", forward)
        return from_low, from_up

    sums = pltpu.VMEM((row_blocks + 1, 8, edge), F32)
    spread = pltpu.VMEM((16 * (rows_dev // width), 2 * halo_width), BF16)
    outside = pltpu.VMEM((2 * halo_blocks + 1, 16, edge), BF16)

    def call(body, in_specs, out_shape, out_specs, scratch, name):
        return pl.pallas_call(
            body,
            out_shape=out_shape,
            in_specs=in_specs,
            out_specs=out_specs,
            scratch_shapes=scratch,
            name=name,
            compiler_params=pltpu.CompilerParams(vmem_limit_bytes=LIMIT),
            cost_estimate=pl.CostEstimate(flops=2 << 30, transcendentals=0, bytes_accessed=1 << 20),
        )

    starts = [start_block]
    for other in range(1, groups):
        pairs = [(i, i ^ other) for i in range(groups)]
        starts.append(lax.ppermute(start_block, "probe", pairs))

    listed = shape((slot_count + UNROLL,), jnp.int32)
    own, halo, sizes = call(
        functools.partial(list_kernel, row_blocks),
        [ANY, ANY, ANY],
        (listed, listed, shape((2,), jnp.int32)),
        (SMEM, SMEM, SMEM),
        [
            pltpu.SMEM(counts.shape, jnp.int32),
            pltpu.SMEM((slot_count,), jnp.int32),
            pltpu.SMEM((slot_count,), jnp.int32),
            pltpu.SemaphoreType.DMA((3,)),
        ],
        "lists",
    )(counts, block_rows, block_cols)
    low, up = call(
        setup_kernel,
        [SMEM, SMEM, VMEM],
        (shape((halo_blocks, edge), F32), shape((halo_blocks, edge), F32)),
        (VMEM, VMEM),
        [sums],
        "setup",
    )(halo, sizes, blocks)
    got_low, got_up = exchange(low, up)
    degree, table = call(
        degree_kernel,
        [SMEM, SMEM, SMEM, VMEM, VMEM],
        (shape((8, rows_dev), F32), shape((width, 2 * halo_width), BF16)),
        (VMEM, VMEM),
        [sums, sums],
        "degree",
    )(own, halo, sizes, blocks, boundary)

    message = shape((16, halo_width), F32)
    vector_shape = shape((probes, rows_dev), F32)
    source_shape = shape((row_blocks + 1, 16, edge), BF16)
    to_low, to_up, vector, scale, source = call(
        first_kernel,
        [SMEM, SMEM] + [VMEM] * (6 + groups),
        (message, message, vector_shape, vector_shape, source_shape),
        (VMEM,) * 5,
        [spread, sums],
        "first",
    )(halo, sizes, blocks, boundary, table, degree, got_low, got_up, *starts)

    vectors = [vector]
    for step in range(STEPS):
        got_low, got_up = exchange(to_low, to_up)
        image = call(
            own_kernel,
            [SMEM, SMEM, VMEM, VMEM],
            vector_shape,
            VMEM,
            [sums],
            f"own{step}",
        )(own, sizes, blocks, source)
        if step + 1 < STEPS:
            to_low, to_up, vector, source = call(
                functools.partial(middle_kernel, SHIFTS[step]),
                [SMEM, SMEM] + [VMEM] * 8,
                (message, message, vector_shape, source_shape),
                (VMEM,) * 4,
                [spread, sums, outside],
                f"middle{step}",
            )(halo, sizes, blocks, boundary, table, vectors[-1], scale, image, got_low, got_up)
        else:
            grams, vector = call(
                functools.partial(last_kernel, SHIFTS[step]),
                [SMEM, SMEM] + [VMEM] * (7 + STEPS),
                (shape((8 * parts, 128), F32), vector_shape),
                (VMEM,) * 2,
                [spread, sums, outside],
                "last",
            )(halo, sizes, blocks, boundary, table, scale, image, got_low, got_up, *vectors)
        vectors.append(vector)
    gathered = lax.all_to_all(grams, "rows", 0, 0, tiled=True)
    return call(
        functools.partial(final_kernel, float(node_total)),
        [VMEM] * (2 + STEPS),
        (
            shape((each, rows_dev), F32),
            shape((STEPS, probes, probes), F32),
            shape((STEPS, probes, probes), F32),
        ),
        (VMEM,) * 3,
        [],
        "final",
    )(gathered, *vectors)


def solution(mesh):
    in_specs = (
        P("probe", "rows"),
        P("rows", None, None),
        P("rows"),
        P("rows"),
        P("rows"),
        P(None, "rows"),
    )
    out_specs = (P("probe", "rows"), P(), P())
    return jax.shard_map(local, mesh=mesh, in_specs=in_specs, out_specs=out_specs, check_vma=False)
```

```python
import functools

import jax
import jax.numpy as jnp
from jax import lax
from jax.experimental import pallas as pl
from jax.experimental.pallas import tpu as pltpu
from jax.sharding import PartitionSpec as P

STEPS = 3
SHIFTS = (0.0, 1.0, 0.0)
UNROLL = 16
LIMIT = 16 << 20
F32 = jnp.float32
BF16 = jnp.bfloat16

SMEM = pl.BlockSpec(memory_space=pltpu.SMEM)
VMEM = pl.BlockSpec(memory_space=pltpu.VMEM)
ANY = pl.BlockSpec(memory_space=pl.ANY)


def dot(a, b, contract):
    return lax.dot_general(a, b, (contract, ((), ())), preferred_element_type=F32)


def exact_dot(a, b, contract):
    return lax.dot_general(
        a, b, (contract, ((), ())), precision=lax.Precision.HIGHEST, preferred_element_type=F32
    )


def for_slots(slots, live, body):
    def group(index, carry):
        entries = []
        for lane in range(UNROLL):
            code = slots[index * UNROLL + lane]
            entries.append((code & 255, (code >> 8) & 255, code >> 16))
        body(entries)
        return carry

    lax.fori_loop(0, (live + UNROLL - 1) // UNROLL, group, 0)


def two_parts(values):
    high = values.astype(BF16).astype(F32)
    return jnp.concatenate([high, values - high], axis=0)


def add_products(entries, tiles, source, totals, forward):
    products = []
    for slot, row, col in entries:
        index = col if forward else row
        got = dot(source[index], tiles[slot], ((1,), (1,)) if forward else ((1,), (0,)))
        products.append(got[: got.shape[0] // 2] + got[got.shape[0] // 2 :])
    for (slot, row, col), got in zip(entries, products):
        index = row if forward else col
        totals[index] = totals[index] + got


def fill_one_hot(bound, table):
    width = table.shape[0]
    halo = bound.shape[1]
    for part in range(2):
        for begin in range(0, halo, width):
            low = bound[part : part + 1, begin : begin + width] & (width - 1)
            hit = lax.broadcasted_iota(jnp.int32, (width, width), 0) == low
            table[:, part * halo + begin : part * halo + begin + width] = jnp.where(
                hit, 1.0, 0.0
            ).astype(BF16)


def add_boundary(bound, table, spread, values):
    width = table.shape[0]
    shift = width.bit_length() - 1
    high_count = spread.shape[0] // 16
    high = jnp.concatenate([bound[0:1, :], bound[1:2, :]], axis=1) >> shift
    stacked = two_parts(values)
    for index in range(high_count):
        spread[16 * index : 16 * index + 16, :] = jnp.where(high == index, stacked, 0.0).astype(BF16)
    got = dot(spread[...], table[...], ((1,), (1,)))
    return [got[16 * i : 16 * i + 8] + got[16 * i + 8 : 16 * i + 16] for i in range(high_count)]


def pick_boundary(bound, table, source, out_low, out_up):
    width = table.shape[0]
    shift = width.bit_length() - 1
    halo = bound.shape[1]
    edge = source.shape[2]
    ratio = width // edge
    high_count = (source.shape[0] - 1) // ratio
    rows = jnp.concatenate(
        [
            jnp.concatenate([source[ratio * i + j] for j in range(ratio)], axis=1)
            for i in range(high_count)
        ],
        axis=0,
    )
    for part, out in enumerate((out_low, out_up)):
        for begin in range(0, halo, width):
            got = dot(rows, table[:, part * halo + begin : part * halo + begin + width], ((1,), (0,)))
            high = bound[part : part + 1, begin : begin + width] >> shift
            total = jnp.zeros((8, width), F32)
            for index in range(high_count):
                one = got[16 * index : 16 * index + 8] + got[16 * index + 8 : 16 * index + 16]
                total = total + jnp.where(high == index, one, 0.0)
            out[0:8, begin : begin + width] = total


def each_live(counts, block_rows, block_cols, spare_row, spare_col, body):
    live = counts[0]

    def group(index, carry):
        entries = []
        for lane in range(UNROLL):
            slot = index * UNROLL + lane
            dead = slot >= live
            entries.append(
                (
                    slot,
                    jnp.where(dead, spare_row, block_rows[slot]),
                    jnp.where(dead, spare_col, block_cols[slot]),
                )
            )
        return body(entries, carry)

    return lax.fori_loop(0, (live + UNROLL - 1) // UNROLL, group, (0, 0))


def setup_kernel(counts, block_rows, block_cols, tiles, table, low, up, inner, sums):
    edge = tiles.shape[1]
    halo_blocks = low.shape[0]
    row_blocks = inner.shape[0]
    sums[...] = jnp.zeros_like(sums)

    def add(entries, carry):
        parts = [
            jnp.sum(tiles[slot].astype(F32).reshape(edge // 8, 8, edge), axis=0)
            for slot, row, col in entries
        ]
        for (slot, row, col), part in zip(entries, parts):
            sums[col] = sums[col] + part
        return carry

    each_live(counts, block_rows, block_cols, row_blocks, sums.shape[0] - 1, add)
    for out, base in ((inner, 0), (low, row_blocks), (up, row_blocks + halo_blocks)):
        for index in range(out.shape[0]):
            out[index : index + 1, :] = jnp.sum(sums[base + index], axis=0, keepdims=True)


def degree_kernel(
    counts, block_rows, block_cols, tiles, inner, own, halo, sizes, degree, row_sums
):
    edge = tiles.shape[1]
    row_blocks = inner.shape[0]
    row_sums[...] = jnp.zeros_like(row_sums)
    ones = jnp.ones((16, edge), BF16)

    def add(entries, carry):
        own_count, halo_count = carry
        for slot, row, col in entries:
            outside = (col >= row_blocks).astype(jnp.int32)
            alive = (row < row_blocks).astype(jnp.int32)
            code = slot | (row << 8) | ((col - row_blocks * outside) << 16)
            own[own_count] = code
            halo[halo_count] = code
            own_count = own_count + alive * (1 - outside)
            halo_count = halo_count + alive * outside
        parts = [dot(ones, tiles[slot], ((1,), (1,)))[0:8] for slot, row, col in entries]
        for (slot, row, col), part in zip(entries, parts):
            row_sums[row] = row_sums[row] + part
        return own_count, halo_count

    own_count, halo_count = each_live(counts, block_rows, block_cols, row_blocks, 0, add)
    empty = (row_blocks << 8) | (row_blocks << 16)
    for lane in range(UNROLL):
        own[own_count + lane] = empty
        halo[halo_count + lane] = empty
    sizes[0] = own_count
    sizes[1] = halo_count
    for index in range(row_blocks):
        degree[:, index * edge : (index + 1) * edge] = (
            1.0 + row_sums[index] + inner[index : index + 1, :]
        )


def send_products(sizes, halo, tiles, bound, table, vector, scale, source, sums, out_low, out_up):
    edge = source.shape[2]
    row_blocks = source.shape[0] - 1
    half = row_blocks // 2
    for index in range(row_blocks):
        part = slice(index * edge, (index + 1) * edge)
        source[index] = two_parts(scale[:, part] * vector[:, part]).astype(BF16)
    source[row_blocks] = jnp.zeros_like(source[row_blocks])
    sums[...] = jnp.zeros_like(sums)
    for_slots(
        halo, sizes[1], lambda entries: add_products(entries, tiles, source, sums, False)
    )
    for index in range(half):
        part = slice(index * edge, (index + 1) * edge)
        out_low[8:16, part] = sums[index]
        out_up[8:16, part] = sums[half + index]
    pick_boundary(bound, table, source, out_low, out_up)


def first_kernel(
    halo, sizes, tiles, bound, table, degree, got_low, got_up, *rest
):
    starts = rest[:-7]
    out_low, out_up, vector, scale, source, spread, sums = rest[-7:]
    each = starts[0].shape[0]
    place = lax.axis_index("probe")
    for block in range(len(starts)):
        rows = starts[0][...]
        for other in range(1, len(starts)):
            rows = jnp.where(place == (block ^ other), starts[other][...], rows)
        vector[block * each : (block + 1) * each, :] = rows
    received = jnp.concatenate(
        [got[i : i + 1, :] for got in (got_low, got_up) for i in range(got.shape[0])], axis=1
    )
    received = jnp.broadcast_to(received, (8, received.shape[1]))
    width = table.shape[0]
    for index, part in enumerate(add_boundary(bound, table, spread, received)):
        cols = slice(index * width, (index + 1) * width)
        total = degree[:, cols] + part
        root = lax.rsqrt(total)
        scale[:, cols] = root * (1.5 - 0.5 * total * root * root)
    send_products(sizes, halo, tiles, bound, table, vector, scale, source, sums, out_low, out_up)


def own_kernel(own, sizes, tiles, source, image, sums):
    edge = tiles.shape[1]
    sums[...] = jnp.zeros_like(sums)

    def add(entries):
        add_products(entries, tiles, source, sums, True)
        add_products(entries, tiles, source, sums, False)

    for_slots(own, sizes[0], add)
    for index in range(sums.shape[0] - 1):
        image[:, index * edge : (index + 1) * edge] = sums[index]


def next_vector(
    shift, halo, sizes, tiles, bound, table, previous, scale, image, got_low, got_up,
    vector, spread, sums, outside,
):
    edge = tiles.shape[1]
    halo_blocks = got_low.shape[1] // edge
    for index in range(halo_blocks):
        part = slice(index * edge, (index + 1) * edge)
        outside[index] = two_parts(got_low[0:8, part]).astype(BF16)
        outside[halo_blocks + index] = two_parts(got_up[0:8, part]).astype(BF16)
    outside[2 * halo_blocks] = jnp.zeros_like(outside[0])
    received = jnp.concatenate([got_low[8:16, :], got_up[8:16, :]], axis=1)
    added = add_boundary(bound, table, spread, received)
    width = table.shape[0]
    ratio = width // edge
    for index in range(sums.shape[0] - 1):
        part = slice((index % ratio) * edge, (index % ratio + 1) * edge)
        sums[index] = (
            added[index // ratio][:, part] + image[:, index * edge : (index + 1) * edge]
        )
    for_slots(
        halo, sizes[1], lambda entries: add_products(entries, tiles, outside, sums, True)
    )
    for index in range(sums.shape[0] - 1):
        part = slice(index * edge, (index + 1) * edge)
        old = previous[:, part]
        root = scale[:, part]
        vector[:, part] = root * (root * old) + root * sums[index] - shift * old


def middle_kernel(
    shift, halo, sizes, tiles, bound, table, previous, scale, image, got_low, got_up,
    out_low, out_up, vector, source, spread, sums, outside,
):
    next_vector(
        shift, halo, sizes, tiles, bound, table, previous, scale, image, got_low, got_up,
        vector, spread, sums, outside,
    )
    send_products(sizes, halo, tiles, bound, table, vector, scale, source, sums, out_low, out_up)


def three_parts(values):
    high = values.astype(BF16)
    rest = values - high.astype(F32)
    middle = rest.astype(BF16)
    return [high, middle, (rest - middle.astype(F32)).astype(BF16)]


def last_kernel(
    shift, halo, sizes, tiles, bound, table, scale, image, got_low, got_up, *rest
):
    vectors = rest[:STEPS]
    gram, vector, spread, sums, outside = rest[STEPS:]
    next_vector(
        shift, halo, sizes, tiles, bound, table, vectors[-1], scale, image, got_low, got_up,
        vector, spread, sums, outside,
    )
    basis = jnp.concatenate([one[...] for one in vectors] + [vector[...]], axis=0)
    size = basis.shape[0]
    parts = jnp.concatenate(three_parts(basis), axis=0)
    wide = dot(parts, parts, ((1,), (1,)))
    total = sum(
        wide[i * size : (i + 1) * size, j * size : (j + 1) * size]
        for i in reversed(range(3))
        for j in reversed(range(3))
    )
    packed = jnp.concatenate([total[8 * i : 8 * i + 8, :] for i in range(size // 8)], axis=1)
    for copy in range(gram.shape[0] // 8):
        gram[8 * copy : 8 * copy + 8, :] = packed


def final_kernel(node_total, grams, *rest):
    vectors = rest[: STEPS + 1]
    basis, alphas, betas = rest[STEPS + 1 :]
    size = 8 * (STEPS + 1)
    packed = grams[0:8, :]
    for copy in range(1, grams.shape[0] // 8):
        packed = packed + grams[8 * copy : 8 * copy + 8, :]
    packed = packed * (1.0 / node_total)
    gram = jnp.concatenate(
        [packed[:, i * size : (i + 1) * size] for i in range(STEPS + 1)], axis=0
    )
    row_ids = lax.broadcasted_iota(jnp.int32, (size, size), 0)
    col_ids = lax.broadcasted_iota(jnp.int32, (size, size), 1)
    unit = jnp.where(row_ids == col_ids, 1.0, 0.0)
    work = jnp.concatenate([gram, unit], axis=1)
    rows = lax.broadcasted_iota(jnp.int32, (size, 2 * size), 0)
    pivots = jnp.ones((size, 2 * size), F32)
    for begin in range(0, size, 8):
        columns = [
            jnp.broadcast_to(work[:, begin + c : begin + c + 1], (size, 2 * size)) for c in range(8)
        ]
        for c in range(8):
            k = begin + c
            pivot = columns[c][k : k + 1, :]
            pivots = jnp.where(rows == k, pivot, pivots)
            factor = jnp.where(rows > k, columns[c] * (1.0 / pivot), 0.0)
            work = work - factor * work[k : k + 1, :]
            for d in range(c + 1, 8):
                columns[d] = columns[d] - factor * columns[d][k : k + 1, :]
    work = work / jnp.sqrt(pivots)
    upper = jnp.where(row_ids <= col_ids, work[:, :size], 0.0)
    inverse = work[:, size:]
    own = jnp.where(row_ids // 8 == col_ids // 8, inverse, 0.0)
    moved = jnp.concatenate(
        [jnp.zeros((8, size), F32)]
        + [
            jnp.concatenate(
                [jnp.zeros((8, 8), F32), own[8 * i : 8 * i + 8, : size - 8]], axis=1
            )
            for i in range(STEPS)
        ],
        axis=0,
    )
    by_last = exact_dot(moved, upper, ((1,), (1,)))
    by_own = exact_dot(own, upper, ((1,), (1,)))
    small = unit[0:8, 0:8]

    def piece(table, i, j):
        return table[8 * i : 8 * i + 8, 8 * j : 8 * j + 8]

    for j in range(STEPS):
        beta = piece(by_last, j + 1, j + 1)
        alpha = (1.0 - SHIFTS[j]) * small - piece(by_last, j + 1, j)
        if j:
            alpha = alpha + exact_dot(piece(by_own, j, j - 1), piece(by_last, j, j), ((1,), (0,)))
        betas[j] = jnp.where(row_ids[0:8, 0:8] >= col_ids[0:8, 0:8], beta, 0.0)
        alphas[j] = alpha
    last = inverse[size - 8 :, :] * (-1.0) ** STEPS
    each = basis.shape[0]
    place = lax.axis_index("probe")
    ids = lax.broadcasted_iota(jnp.int32, (8, size), 0)
    chosen = jnp.zeros((8, size), F32)
    for index in range(each):
        line = jnp.sum(jnp.where(ids == place * each + index, last, 0.0), axis=0, keepdims=True)
        chosen = jnp.where(ids == index, line, chosen)
    total = exact_dot(chosen, jnp.concatenate([one[...] for one in vectors], axis=0), ((1,), (0,)))
    basis[...] = total[0:each]


def local(start_block, blocks, block_rows, block_cols, counts, boundary):
    each, rows_dev = start_block.shape
    slot_count, edge, _ = blocks.shape
    halo_width = boundary.shape[1]
    parts = lax.axis_size("rows")
    groups = lax.axis_size("probe")
    node_total = rows_dev * parts
    row_blocks = rows_dev // edge
    halo_blocks = halo_width // edge
    probes = each * groups
    width = 2 * edge
    shape = jax.ShapeDtypeStruct

    forward = [(i, (i + 1) % parts) for i in range(parts)]
    backward = [(target, source) for source, target in forward]

    def exchange(to_low, to_up):
        from_up = lax.ppermute(to_low, "rows", backward)
        from_low = lax.ppermute(to_up, "rows", forward)
        return from_low, from_up

    sums = pltpu.VMEM((row_blocks + 1, 8, edge), F32)
    spread = pltpu.VMEM((16 * (rows_dev // width), 2 * halo_width), BF16)
    outside = pltpu.VMEM((2 * halo_blocks + 1, 16, edge), BF16)

    def call(body, in_specs, out_shape, out_specs, scratch, name):
        return pl.pallas_call(
            body,
            out_shape=out_shape,
            in_specs=in_specs,
            out_specs=out_specs,
            scratch_shapes=scratch,
            name=name,
            compiler_params=pltpu.CompilerParams(vmem_limit_bytes=LIMIT),
            cost_estimate=pl.CostEstimate(flops=2 << 30, transcendentals=0, bytes_accessed=1 << 20),
        )

    starts = [start_block]
    for other in range(1, groups):
        pairs = [(i, i ^ other) for i in range(groups)]
        starts.append(lax.ppermute(start_block, "probe", pairs))
    table = call(
        fill_one_hot, [VMEM], shape((width, 2 * halo_width), BF16), VMEM, [], "table"
    )(boundary)
    low, up, inner = call(
        setup_kernel,
        [SMEM, SMEM, SMEM, VMEM, ANY],
        (
            shape((halo_blocks, edge), F32),
            shape((halo_blocks, edge), F32),
            shape((row_blocks, edge), F32),
        ),
        (VMEM,) * 3,
        [pltpu.VMEM((row_blocks + 2 * halo_blocks + 1, 8, edge), F32)],
        "setup",
    )(counts, block_rows, block_cols, blocks, table)
    got_low, got_up = exchange(low, up)
    listed = shape((slot_count + UNROLL,), jnp.int32)
    own, halo, sizes, degree = call(
        degree_kernel,
        [SMEM, SMEM, SMEM, VMEM, VMEM],
        (listed, listed, shape((2,), jnp.int32), shape((8, rows_dev), F32)),
        (SMEM, SMEM, SMEM, VMEM),
        [sums],
        "degree",
    )(counts, block_rows, block_cols, blocks, inner)

    message = shape((16, halo_width), F32)
    vector_shape = shape((probes, rows_dev), F32)
    source_shape = shape((row_blocks + 1, 16, edge), BF16)
    to_low, to_up, vector, scale, source = call(
        first_kernel,
        [SMEM, SMEM] + [VMEM] * (6 + groups),
        (message, message, vector_shape, vector_shape, source_shape),
        (VMEM,) * 5,
        [spread, sums],
        "first",
    )(halo, sizes, blocks, boundary, table, degree, got_low, got_up, *starts)

    vectors = [vector]
    for step in range(STEPS):
        got_low, got_up = exchange(to_low, to_up)
        image = call(
            own_kernel,
            [SMEM, SMEM, VMEM, VMEM],
            vector_shape,
            VMEM,
            [sums],
            f"own{step}",
        )(own, sizes, blocks, source)
        if step + 1 < STEPS:
            to_low, to_up, vector, source = call(
                functools.partial(middle_kernel, SHIFTS[step]),
                [SMEM, SMEM] + [VMEM] * 8,
                (message, message, vector_shape, source_shape),
                (VMEM,) * 4,
                [spread, sums, outside],
                f"middle{step}",
            )(halo, sizes, blocks, boundary, table, vectors[-1], scale, image, got_low, got_up)
        else:
            grams, vector = call(
                functools.partial(last_kernel, SHIFTS[step]),
                [SMEM, SMEM] + [VMEM] * (7 + STEPS),
                (shape((8 * parts, 128), F32), vector_shape),
                (VMEM,) * 2,
                [spread, sums, outside],
                "last",
            )(halo, sizes, blocks, boundary, table, scale, image, got_low, got_up, *vectors)
        vectors.append(vector)
    gathered = lax.all_to_all(grams, "rows", 0, 0, tiled=True)
    return call(
        functools.partial(final_kernel, float(node_total)),
        [VMEM] * (2 + STEPS),
        (
            shape((each, rows_dev), F32),
            shape((STEPS, probes, probes), F32),
            shape((STEPS, probes, probes), F32),
        ),
        (VMEM,) * 3,
        [],
        "final",
    )(gathered, *vectors)


def solution(mesh):
    in_specs = (
        P("probe", "rows"),
        P("rows", None, None),
        P("rows"),
        P("rows"),
        P("rows"),
        P(None, "rows"),
    )
    out_specs = (P("probe", "rows"), P(), P())
    return jax.shard_map(local, mesh=mesh, in_specs=in_specs, out_specs=out_specs, check_vma=False)
```

```python
import functools

import jax
import jax.numpy as jnp
from jax import lax
from jax.experimental import pallas as pl
from jax.experimental.pallas import tpu as pltpu
from jax.sharding import PartitionSpec as P


STEPS = 3
SHIFTS = (0.0, 1.0, 0.0)
WIDE = 32
NARROW = 8
LIMIT = 16 << 20
F32 = jnp.float32
BF16 = jnp.bfloat16

SMEM = pl.BlockSpec(memory_space=pltpu.SMEM)
VMEM = pl.BlockSpec(memory_space=pltpu.VMEM)
ANY = pl.BlockSpec(memory_space=pl.ANY)


def dot(a, b, contract):
    return lax.dot_general(a, b, (contract, ((), ())), preferred_element_type=F32)


def exact_dot(a, b, contract):
    return lax.dot_general(
        a, b, (contract, ((), ())), precision=lax.Precision.HIGHEST, preferred_element_type=F32
    )


def for_slots(slots, live, body):
    def turns(size, first, count):
        def group(index, carry):
            entries = []
            for lane in range(size):
                code = slots[first + index * size + lane]
                entries.append((code & 255, (code >> 8) & 255, code >> 16))
            body(entries)
            return carry

        lax.fori_loop(0, count, group, 0)

    wide = live // WIDE
    turns(WIDE, 0, wide)
    turns(NARROW, wide * WIDE, (live - wide * WIDE + NARROW - 1) // NARROW)


def two_parts(values):
    high = values.astype(BF16).astype(F32)
    return jnp.concatenate([high, values - high], axis=0)


def add_products(entries, tiles, source, totals, forward):
    products = []
    for slot, row, col in entries:
        index = col if forward else row
        got = dot(source[index], tiles[slot], ((1,), (1,)) if forward else ((1,), (0,)))
        products.append(got if got.shape[0] == 8 else got[0:8] + got[8:16])
    for (slot, row, col), got in zip(entries, products):
        index = row if forward else col
        totals[index] = totals[index] + got


def fill_one_hot(index, table):
    width = table.shape[0]
    for begin in range(0, index.shape[1], width):
        low = index[:, begin : begin + width] & (width - 1)
        hit = lax.broadcasted_iota(jnp.int32, (width, width), 0) == low
        table[:, begin : begin + width] = jnp.where(hit, 1.0, 0.0).astype(BF16)


def index_kernel(bound, low, table, high, hot, place, spread):
    even = lax.axis_index("rows") % 2 == 0
    upper = bound[1:2, :]
    lower = bound[0:1, :]
    index = jnp.concatenate(
        [jnp.where(even, upper, lower), jnp.where(even, lower, upper)], axis=1
    )
    main = hot.shape[1]
    width = table.shape[0]
    shift = width.bit_length() - 1
    rest = table.shape[1] - main
    high[...] = jnp.broadcast_to(index >> shift, high.shape)
    fill_one_hot(index, table)
    entry = lax.broadcasted_iota(jnp.int32, (8, rest), 1) + 1
    stacked = two_parts(entry.astype(F32))
    both = jnp.broadcast_to(index >> shift, (16, index.shape[1]))
    high_count = spread.shape[0] // 16
    for part in range(high_count):
        rows = slice(16 * part, 16 * part + 16)
        hot[rows, :] = jnp.where(both[:, :main] == part, 1.0, 0.0).astype(BF16)
        spread[rows, :] = jnp.where(both[:, main:] == part, stacked, 0.0).astype(BF16)
    got = dot(spread[...], table[:, main:], ((1,), (1,)))
    for part in range(high_count):
        one = got[16 * part : 16 * part + 8] + got[16 * part + 8 : 16 * part + 16]
        place[:, part * width : (part + 1) * width] = (one + 0.5).astype(jnp.int32) - 1


def gathered(code, sources):
    edge = code.shape[1]
    lane = code & (edge - 1)
    block = code >> (edge.bit_length() - 1)
    total = jnp.zeros(code.shape, F32)
    for index, source in enumerate(sources):
        moved = jnp.take_along_axis(source, lane, axis=1, mode="promise_in_bounds")
        total = jnp.where(block == index, moved, total)
    return total


def add_boundary(table, hot, place, spread, values):
    edge = values[0].shape[1]
    main = hot.shape[1]
    width = table.shape[0]
    count = main // edge
    high_count = spread.shape[0] // 16
    for block in range(count):
        cols = slice(block * edge, (block + 1) * edge)
        for index in range(high_count):
            rows = slice(16 * index, 16 * index + 16)
            spread[rows, cols] = hot[rows, cols] * values[block]
    got = dot(spread[...], table[:, :main], ((1,), (1,)))
    last = [value.astype(F32) for value in values[count:]]
    last = [value[0:8] + value[8:16] for value in last]
    result = []
    for index in range(high_count):
        one = got[16 * index : 16 * index + 8] + got[16 * index + 8 : 16 * index + 16]
        for begin in range(0, width, edge):
            cols = slice(index * width + begin, index * width + begin + edge)
            result.append(one[:, begin : begin + edge] + gathered(place[:, cols], last))
    return result


def pick_boundary(table, high, vector, scale, outs):
    width = table.shape[0]
    halo = table.shape[1] // 2
    high_count = vector.shape[1] // width
    rows = jnp.concatenate(
        [
            scale[:, index * width : (index + 1) * width]
            * vector[:, index * width : (index + 1) * width]
            for index in range(high_count)
        ],
        axis=0,
    ).astype(BF16)

    def picked(begin):
        cols = slice(begin, begin + width)
        got = dot(rows, table[:, cols], ((1,), (0,)))
        total = jnp.zeros((8, width), F32)
        for index in range(high_count):
            total = jnp.where(high[:, cols] == index, got[8 * index : 8 * index + 8], total)
        return total

    for side, out in enumerate(outs):
        for begin in range(0, halo // 2, width):
            first = picked(side * halo + begin)
            second = picked(side * halo + halo // 2 + begin)
            out[:, halo + begin : halo + begin + width] = jnp.concatenate(
                [first, second], axis=0
            ).astype(BF16)


def warm_kernel(out):
    out[...] = jnp.zeros_like(out)


def each_live(size, counts, block_rows, block_cols, spare_row, spare_col, body):
    live = counts[0]

    def group(index, carry):
        entries = []
        for lane in range(size):
            slot = index * size + lane
            dead = slot >= live
            entries.append(
                (
                    slot,
                    jnp.where(dead, spare_row, block_rows[slot]),
                    jnp.where(dead, spare_col, block_cols[slot]),
                )
            )
        return body(entries, carry)

    return lax.fori_loop(0, (live + size - 1) // size, group, (0, 0))


def by_side(col, row_blocks):
    even = 1 - lax.axis_index("rows") % 2
    return (col - row_blocks + even * (row_blocks // 2)) & (row_blocks - 1)


def setup_kernel(
    counts_in, block_rows, block_cols, tiles, warm, first, second, inner, sums, counts, sem
):
    copy = pltpu.make_async_copy(counts_in, counts, sem.at[0])
    copy.start()
    edge = tiles.shape[1]
    halo_blocks = first.shape[0]
    row_blocks = inner.shape[0]
    sums[...] = jnp.zeros_like(sums)

    def add(entries, carry):
        parts = [
            jnp.sum(tiles[slot].astype(F32).reshape(edge // 8, 8, edge), axis=0)
            for slot, row, col in entries
        ]
        for (slot, row, col), part in zip(entries, parts):
            inside = jnp.logical_or(col < row_blocks, col == sums.shape[0] - 1)
            index = jnp.where(inside, col, row_blocks + by_side(col, row_blocks))
            sums[index] = sums[index] + part
        return carry

    copy.wait()
    each_live(16, counts, block_rows, block_cols, row_blocks, sums.shape[0] - 1, add)
    for out, base in ((inner, 0), (first, row_blocks), (second, row_blocks + halo_blocks)):
        for index in range(out.shape[0]):
            out[index : index + 1, :] = jnp.sum(sums[base + index], axis=0, keepdims=True)


def degree_kernel(
    counts_in, block_rows, block_cols, tiles, inner, own, halo, sizes, degree, row_sums, counts, sem
):
    copy = pltpu.make_async_copy(counts_in, counts, sem.at[0])
    copy.start()
    edge = tiles.shape[1]
    row_blocks = inner.shape[0]
    row_sums[...] = jnp.zeros_like(row_sums)
    ones = jnp.ones((16, edge), BF16)

    def add(entries, carry):
        own_count, halo_count = carry
        for slot, row, col in entries:
            outside = (col >= row_blocks).astype(jnp.int32)
            alive = (row < row_blocks).astype(jnp.int32)
            index = jnp.where(col >= row_blocks, by_side(col, row_blocks), col)
            code = slot | (row << 8) | (index << 16)
            own[own_count] = code
            halo[halo_count] = code
            own_count = own_count + alive * (1 - outside)
            halo_count = halo_count + alive * outside
        parts = [dot(ones, tiles[slot], ((1,), (1,)))[0:8] for slot, row, col in entries]
        for (slot, row, col), part in zip(entries, parts):
            row_sums[row] = row_sums[row] + part
        return own_count, halo_count

    copy.wait()
    own_count, halo_count = each_live(WIDE, counts, block_rows, block_cols, row_blocks, 0, add)
    empty = (row_blocks << 8) | (row_blocks << 16)
    for lane in range(NARROW):
        own[own_count + lane] = empty
        halo[halo_count + lane] = empty
    sizes[0] = own_count
    sizes[1] = halo_count
    for index in range(row_blocks):
        degree[:, index * edge : (index + 1) * edge] = (
            1.0 + row_sums[index] + inner[index : index + 1, :]
        )


class Lists:
    def __init__(self, halo_in, sizes_in, halo, sizes, sems):
        self.halo, self.sizes = halo, sizes
        self.copies = [
            pltpu.make_async_copy(halo_in, halo, sems.at[0]),
            pltpu.make_async_copy(sizes_in, sizes, sems.at[1]),
        ]
        for copy in self.copies:
            copy.start()

    def each(self, body):
        for copy in self.copies:
            copy.wait()
        self.copies = []
        for_slots(self.halo, self.sizes[1], body)


def send_products(lists, tiles, looks, vector, scale, source, sums, outs):
    edge = source.shape[2]
    row_blocks = source.shape[0] - 1
    half = row_blocks // 2
    for index in range(row_blocks):
        part = slice(index * edge, (index + 1) * edge)
        source[index] = two_parts(scale[:, part] * vector[:, part]).astype(BF16)
    source[row_blocks] = jnp.zeros_like(source[row_blocks])
    sums[...] = jnp.zeros_like(sums)
    lists.each(lambda entries: add_products(entries, tiles, source, sums, False))
    for side, out in enumerate(outs):
        for index in range(half):
            out[:, index * edge : (index + 1) * edge] = two_parts(
                sums[side * half + index]
            ).astype(BF16)
    pick_boundary(*looks, vector, scale, outs)


def first_kernel(
    halo_in, sizes_in, tiles, table, high, hot, place, degree, got_first, got_second, *rest
):
    starts = rest[:-10]
    out_first, out_second, vector, scale, source, spread, sums, halo, sizes, sems = rest[-10:]
    lists = Lists(halo_in, sizes_in, halo, sizes, sems)
    edge = tiles.shape[1]
    each = starts[0].shape[0]
    group = lax.axis_index("probe")
    for block in range(len(starts)):
        rows = starts[0][...]
        for other in range(1, len(starts)):
            rows = jnp.where(group == (block ^ other), starts[other][...], rows)
        vector[block * each : (block + 1) * each, :] = rows
    values = [
        two_parts(jnp.broadcast_to(got[i : i + 1, :], (8, edge))).astype(BF16)
        for got in (got_first, got_second)
        for i in range(got.shape[0])
    ]
    for index, part in enumerate(add_boundary(table, hot, place, spread, values)):
        cols = slice(index * edge, (index + 1) * edge)
        total = degree[:, cols] + part
        root = lax.rsqrt(total)
        scale[:, cols] = root * (1.5 - 0.5 * total * root * root)
    send_products(
        lists, tiles, (table, high), vector, scale, source, sums, (out_first, out_second)
    )


def own_kernel(own, sizes, tiles, source, image, sums):
    edge = tiles.shape[1]
    sums[...] = jnp.zeros_like(sums)

    def add(entries):
        add_products(entries, tiles, source, sums, True)
        add_products(entries, tiles, source, sums, False)

    for_slots(own, sizes[0], add)
    for index in range(sums.shape[0] - 1):
        image[:, index * edge : (index + 1) * edge] = sums[index]


def next_vector(
    shift, lists, tiles, looks, previous, scale, image, got_first, got_second,
    vector, spread, sums, outside,
):
    edge = tiles.shape[1]
    halo = looks[0].shape[1] // 2
    halo_blocks = halo // edge
    values = []
    for side, got in enumerate((got_first, got_second)):
        for index in range(halo_blocks):
            half = index // (halo_blocks // 2)
            begin = halo + (index % (halo_blocks // 2)) * edge
            outside[side * halo_blocks + index] = got[8 * half : 8 * half + 8, begin : begin + edge]
            values.append(got[:, index * edge : (index + 1) * edge])
    outside[2 * halo_blocks] = jnp.zeros_like(outside[0])
    for index, added in enumerate(add_boundary(*looks, spread, values)):
        sums[index] = added + image[:, index * edge : (index + 1) * edge]
    lists.each(lambda entries: add_products(entries, tiles, outside, sums, True))
    for index in range(sums.shape[0] - 1):
        part = slice(index * edge, (index + 1) * edge)
        old = previous[:, part]
        root = scale[:, part]
        vector[:, part] = root * (root * old) + root * sums[index] - shift * old


def middle_kernel(
    shift, halo_in, sizes_in, tiles, table, high, hot, place, previous, scale, image,
    got_first, got_second, out_first, out_second, vector, source,
    spread, sums, outside, halo, sizes, sems,
):
    lists = Lists(halo_in, sizes_in, halo, sizes, sems)
    next_vector(
        shift, lists, tiles, (table, hot, place), previous, scale, image, got_first, got_second,
        vector, spread, sums, outside,
    )
    send_products(
        lists, tiles, (table, high), vector, scale, source, sums, (out_first, out_second)
    )


def three_parts(values):
    high = values.astype(BF16)
    rest = values - high.astype(F32)
    middle = rest.astype(BF16)
    return [high, middle, (rest - middle.astype(F32)).astype(BF16)]


def last_kernel(
    shift, halo_in, sizes_in, tiles, table, hot, place, scale, image, got_first, got_second, *rest
):
    vectors = rest[:STEPS]
    gram, vector, spread, sums, outside, halo, sizes, sems = rest[STEPS:]
    lists = Lists(halo_in, sizes_in, halo, sizes, sems)
    next_vector(
        shift, lists, tiles, (table, hot, place), vectors[-1], scale, image,
        got_first, got_second, vector, spread, sums, outside,
    )
    basis = jnp.concatenate([one[...] for one in vectors] + [vector[...]], axis=0)
    size = basis.shape[0]
    parts = jnp.concatenate(three_parts(basis), axis=0)
    wide = dot(parts, parts, ((1,), (1,)))
    total = sum(
        wide[i * size : (i + 1) * size, j * size : (j + 1) * size]
        for i in reversed(range(3))
        for j in reversed(range(3))
    )
    packed = jnp.concatenate([total[8 * i : 8 * i + 8, :] for i in range(size // 8)], axis=1)
    for copy in range(gram.shape[0] // 8):
        gram[8 * copy : 8 * copy + 8, :] = packed


def final_kernel(node_total, grams, *rest):
    vectors = rest[: STEPS + 1]
    basis, alphas, betas = rest[STEPS + 1 :]
    size = 8 * (STEPS + 1)
    packed = grams[0:8, :]
    for copy in range(1, grams.shape[0] // 8):
        packed = packed + grams[8 * copy : 8 * copy + 8, :]
    packed = packed * (1.0 / node_total)
    gram = jnp.concatenate(
        [packed[:, i * size : (i + 1) * size] for i in range(STEPS + 1)], axis=0
    )
    row_ids = lax.broadcasted_iota(jnp.int32, (size, size), 0)
    col_ids = lax.broadcasted_iota(jnp.int32, (size, size), 1)
    unit = jnp.where(row_ids == col_ids, 1.0, 0.0)
    work = jnp.concatenate([gram, unit], axis=1)
    rows = lax.broadcasted_iota(jnp.int32, (size, 2 * size), 0)
    pivots = jnp.ones((size, 2 * size), F32)
    for begin in range(0, size, 8):
        columns = [
            jnp.broadcast_to(work[:, begin + c : begin + c + 1], (size, 2 * size)) for c in range(8)
        ]
        for c in range(8):
            k = begin + c
            pivot = columns[c][k : k + 1, :]
            pivots = jnp.where(rows == k, pivot, pivots)
            factor = jnp.where(rows > k, columns[c] * (1.0 / pivot), 0.0)
            work = work - factor * work[k : k + 1, :]
            for d in range(c + 1, 8):
                columns[d] = columns[d] - factor * columns[d][k : k + 1, :]
    work = work / jnp.sqrt(pivots)
    upper = jnp.where(row_ids <= col_ids, work[:, :size], 0.0)
    inverse = work[:, size:]
    own = jnp.where(row_ids // 8 == col_ids // 8, inverse, 0.0)
    moved = jnp.concatenate(
        [jnp.zeros((8, size), F32)]
        + [
            jnp.concatenate(
                [jnp.zeros((8, 8), F32), own[8 * i : 8 * i + 8, : size - 8]], axis=1
            )
            for i in range(STEPS)
        ],
        axis=0,
    )
    by_last = exact_dot(moved, upper, ((1,), (1,)))
    by_own = exact_dot(own, upper, ((1,), (1,)))
    small = unit[0:8, 0:8]

    def piece(table, i, j):
        return table[8 * i : 8 * i + 8, 8 * j : 8 * j + 8]

    for j in range(STEPS):
        beta = piece(by_last, j + 1, j + 1)
        alpha = (1.0 - SHIFTS[j]) * small - piece(by_last, j + 1, j)
        if j:
            alpha = alpha + exact_dot(piece(by_own, j, j - 1), piece(by_last, j, j), ((1,), (0,)))
        betas[j] = jnp.where(row_ids[0:8, 0:8] >= col_ids[0:8, 0:8], beta, 0.0)
        alphas[j] = alpha
    last = inverse[size - 8 :, :] * (-1.0) ** STEPS
    each = basis.shape[0]
    place = lax.axis_index("probe")
    ids = lax.broadcasted_iota(jnp.int32, (8, size), 0)
    chosen = jnp.zeros((8, size), F32)
    for index in range(each):
        line = jnp.sum(jnp.where(ids == place * each + index, last, 0.0), axis=0, keepdims=True)
        chosen = jnp.where(ids == index, line, chosen)
    total = exact_dot(chosen, jnp.concatenate([one[...] for one in vectors], axis=0), ((1,), (0,)))
    basis[...] = total[0:each]


def local(start_block, blocks, block_rows, block_cols, counts, boundary):
    each, rows_dev = start_block.shape
    slot_count, edge, _ = blocks.shape
    halo_width = boundary.shape[1]
    parts = lax.axis_size("rows")
    groups = lax.axis_size("probe")
    node_total = rows_dev * parts
    row_blocks = rows_dev // edge
    halo_blocks = halo_width // edge
    probes = each * groups
    width = 2 * edge
    shape = jax.ShapeDtypeStruct

    if parts % 2:
        raise ValueError("odd ring")
    matchings = (
        [(i, i ^ 1) for i in range(parts)],
        [(i, (i + 1) % parts if i % 2 else (i - 1) % parts) for i in range(parts)],
    )

    def exchange(first, second):
        got_second = lax.ppermute(second, "rows", matchings[1])
        got_first = lax.ppermute(first, "rows", matchings[0])
        return got_first, got_second

    listed = (slot_count + NARROW,)
    sums = pltpu.VMEM((row_blocks + 1, 8, edge), F32)
    outside = pltpu.VMEM((2 * halo_blocks + 1, 8, edge), BF16)
    counted = [pltpu.SMEM(counts.shape, jnp.int32), pltpu.SemaphoreType.DMA((1,))]
    fetched = [
        pltpu.SMEM(listed, jnp.int32),
        pltpu.SMEM((2,), jnp.int32),
        pltpu.SemaphoreType.DMA((2,)),
    ]

    def call(body, in_specs, out_shape, out_specs, scratch):
        return pl.pallas_call(
            body,
            out_shape=out_shape,
            in_specs=in_specs,
            out_specs=out_specs,
            scratch_shapes=scratch,
            compiler_params=pltpu.CompilerParams(vmem_limit_bytes=LIMIT),
            cost_estimate=pl.CostEstimate(flops=2 << 30, transcendentals=0, bytes_accessed=1 << 20),
        )

    starts = [start_block]
    for other in range(1, groups):
        pairs = [(i, i ^ other) for i in range(groups)]
        starts.append(lax.ppermute(start_block, "probe", pairs))
    warm = call(warm_kernel, [], shape((8, 128), F32), VMEM, [])()
    low, up, inner = call(
        setup_kernel,
        [VMEM, SMEM, SMEM, VMEM, ANY],
        (
            shape((halo_blocks, edge), F32),
            shape((halo_blocks, edge), F32),
            shape((row_blocks, edge), F32),
        ),
        (VMEM,) * 3,
        [pltpu.VMEM((row_blocks + 2 * halo_blocks + 1, 8, edge), F32)] + counted,
    )(counts, block_rows, block_cols, blocks, warm)
    got = exchange(low, up)
    rest = min(halo_width, 2 * halo_width * 7 // 16 // width * width)
    main = 2 * halo_width - rest
    high_rows = 16 * (rows_dev // width)
    table, high, hot, place = call(
        index_kernel,
        [VMEM, ANY],
        (
            shape((width, 2 * halo_width), BF16),
            shape((8, 2 * halo_width), jnp.int32),
            shape((high_rows, main), BF16),
            shape((8, rows_dev), jnp.int32),
        ),
        (VMEM,) * 4,
        [pltpu.VMEM((high_rows, rest), BF16)],
    )(boundary, low)
    spread = pltpu.VMEM((high_rows, main), BF16)
    own, halo, sizes, degree = call(
        degree_kernel,
        [VMEM, SMEM, SMEM, VMEM, VMEM],
        (
            shape(listed, jnp.int32),
            shape(listed, jnp.int32),
            shape((2,), jnp.int32),
            shape((8, rows_dev), F32),
        ),
        (SMEM, SMEM, SMEM, VMEM),
        [sums] + counted,
    )(counts, block_rows, block_cols, blocks, inner)

    message = shape((16, halo_width + halo_width // 2), BF16)
    vector_shape = shape((probes, rows_dev), F32)
    source_shape = shape((row_blocks + 1, 16, edge), BF16)
    first, second, vector, scale, source = call(
        first_kernel,
        [ANY, ANY] + [VMEM] * (8 + groups),
        (message, message, vector_shape, vector_shape, source_shape),
        (VMEM,) * 5,
        [spread, sums] + fetched,
    )(halo, sizes, blocks, table, high, hot, place, degree, *got, *starts)

    vectors = [vector]
    for step in range(STEPS):
        got = exchange(first, second)
        image = call(
            own_kernel, [SMEM, SMEM, VMEM, VMEM], vector_shape, VMEM, [sums]
        )(own, sizes, blocks, source)
        if step + 1 < STEPS:
            first, second, vector, source = call(
                functools.partial(middle_kernel, SHIFTS[step]),
                [ANY, ANY] + [VMEM] * 10,
                (message, message, vector_shape, source_shape),
                (VMEM,) * 4,
                [spread, sums, outside] + fetched,
            )(halo, sizes, blocks, table, high, hot, place, vectors[-1], scale, image, *got)
        else:
            grams, vector = call(
                functools.partial(last_kernel, SHIFTS[step]),
                [ANY, ANY] + [VMEM] * (8 + STEPS),
                (shape((8 * parts, 128), F32), vector_shape),
                (VMEM,) * 2,
                [spread, sums, outside] + fetched,
            )(halo, sizes, blocks, table, hot, place, scale, image, *got, *vectors)
        vectors.append(vector)
    gathered = lax.all_to_all(grams, "rows", 0, 0, tiled=True)
    return call(
        functools.partial(final_kernel, float(node_total)),
        [VMEM] * (2 + STEPS),
        (
            shape((each, rows_dev), F32),
            shape((STEPS, probes, probes), F32),
            shape((STEPS, probes, probes), F32),
        ),
        (VMEM,) * 3,
        [],
    )(gathered, *vectors)


def solution(mesh):
    in_specs = (
        P("probe", "rows"),
        P("rows", None, None),
        P("rows"),
        P("rows"),
        P("rows"),
        P(None, "rows"),
    )
    out_specs = (P("probe", "rows"), P(), P())
    return jax.shard_map(local, mesh=mesh, in_specs=in_specs, out_specs=out_specs, check_vma=False)
```

```python
import functools

import jax
import jax.numpy as jnp
from jax import lax
from jax.experimental import pallas as pl
from jax.experimental.pallas import tpu as pltpu
from jax.sharding import PartitionSpec as P


STEPS = 3
SHIFTS = (0.0, 1.0, 0.0)
WIDE = 32
LIMIT = 16 << 20
F32 = jnp.float32
BF16 = jnp.bfloat16

SMEM = pl.BlockSpec(memory_space=pltpu.SMEM)
VMEM = pl.BlockSpec(memory_space=pltpu.VMEM)
ANY = pl.BlockSpec(memory_space=pl.ANY)


def dot(a, b, contract):
    return lax.dot_general(a, b, (contract, ((), ())), preferred_element_type=F32)


def exact_dot(a, b, contract):
    return lax.dot_general(
        a, b, (contract, ((), ())), precision=lax.Precision.HIGHEST, preferred_element_type=F32
    )


def for_slots(slots, body):
    live = slots[0, slots.shape[1] - 1]

    def turns(size, first, count):
        def group(index, carry):
            entries = []
            for lane in range(size):
                code = slots[0, first + index * size + lane]
                entries.append((code & 255, (code >> 8) & 255, code >> 16))
            body(entries)
            return carry

        lax.fori_loop(0, count, group, 0)

    wide = (live + WIDE // 2 - 1) // WIDE
    left = live - wide * WIDE
    turns(WIDE, 0, wide)
    turns(WIDE // 2, wide * WIDE, (left > WIDE // 4).astype(jnp.int32))
    small = jnp.logical_and(left > 0, left <= WIDE // 4)
    turns(WIDE // 4, wide * WIDE, small.astype(jnp.int32))


def two_parts(values):
    high = values.astype(BF16).astype(F32)
    return jnp.concatenate([high, values - high], axis=0)


def add_products(entries, tiles, source, totals, forward):
    products = []
    for slot, row, col in entries:
        index = col if forward else row
        got = dot(source[index], tiles[slot], ((1,), (1,)) if forward else ((1,), (0,)))
        products.append(got if got.shape[0] == 8 else got[0:8] + got[8:16])
    for (slot, row, col), got in zip(entries, products):
        index = row if forward else col
        totals[index] = totals[index] + got


def fill_one_hot(index, table):
    width = table.shape[0]
    for begin in range(0, index.shape[1], width):
        low = index[:, begin : begin + width] & (width - 1)
        hit = lax.broadcasted_iota(jnp.int32, (width, width), 0) == low
        table[:, begin : begin + width] = jnp.where(hit, 1.0, 0.0).astype(BF16)


def list_slots(live, rows, cols, row_blocks, outputs):
    count = rows.shape[1]
    shape = (8, count)
    lane = lax.broadcasted_iota(jnp.int32, shape, 1)
    row_id = lax.broadcasted_iota(jnp.int32, shape, 0)
    row = jnp.broadcast_to(rows, shape)
    col = jnp.broadcast_to(cols, shape)
    outside = col >= row_blocks
    index = jnp.where(outside, by_side(col, row_blocks), col)
    fields = jnp.where(row_id == 0, lane, jnp.where(row_id == 1, row, index)).astype(F32)
    square = (count, count)
    first = lax.broadcasted_iota(jnp.int32, square, 0)
    second = lax.broadcasted_iota(jnp.int32, square, 1)
    before = jnp.where(first < second, 1.0, 0.0).astype(BF16)
    empty = (row_blocks << 8) | (row_blocks << 16)
    for out, outer in zip(outputs, (False, True)):
        mine = jnp.logical_and(lane < live, outside if outer else jnp.logical_not(outside))
        ones = jnp.where(mine, 1.0, 0.0)
        ahead = dot(ones.astype(BF16), before, ((1,), (0,)))
        total = jnp.sum(ones, axis=1, keepdims=True).astype(jnp.int32)[0:1]
        spot = jnp.where(mine, ahead, -1.0)[0:1]
        moved = jnp.where(
            jnp.broadcast_to(spot, square).T == second.astype(F32), 1.0, 0.0
        ).astype(BF16)
        placed = dot(fields.astype(BF16), moved, ((1,), (0,))).astype(jnp.int32)
        code = placed[0:1] | (placed[1:2] << 8) | (placed[2:3] << 16)
        out[:, :count] = jnp.where(lane[0:1] < total, code, empty)
        out[:, count:] = jnp.where(lane[0:1] == count - 1, total, empty)


def index_kernel(
    counts_in, slot_rows, slot_cols, bound, low, own, halo, table, high, hot, place, spread, counts, sem
):
    copy = pltpu.make_async_copy(counts_in, counts, sem.at[0])
    copy.start()
    even = lax.axis_index("rows") % 2 == 0
    upper = bound[1:2, :]
    lower = bound[0:1, :]
    index = jnp.concatenate(
        [jnp.where(even, upper, lower), jnp.where(even, lower, upper)], axis=1
    )
    main = hot.shape[1]
    width = table.shape[0]
    shift = width.bit_length() - 1
    rest = table.shape[1] - main
    high[...] = jnp.broadcast_to(index >> shift, high.shape)
    fill_one_hot(index, table)
    entry = lax.broadcasted_iota(jnp.int32, (8, rest), 1) + 1
    stacked = two_parts(entry.astype(F32))
    both = jnp.broadcast_to(index >> shift, (16, index.shape[1]))
    high_count = spread.shape[0] // 16
    for part in range(high_count):
        rows = slice(16 * part, 16 * part + 16)
        hot[rows, :] = jnp.where(both[:, :main] == part, 1.0, 0.0).astype(BF16)
        spread[rows, :] = jnp.where(both[:, main:] == part, stacked, 0.0).astype(BF16)
    got = dot(spread[...], table[:, main:], ((1,), (1,)))
    for part in range(high_count):
        one = got[16 * part : 16 * part + 8] + got[16 * part + 8 : 16 * part + 16]
        place[:, part * width : (part + 1) * width] = (one + 0.5).astype(jnp.int32) - 1
    copy.wait()
    row_blocks = place.shape[1] // low.shape[1]
    list_slots(counts[0], slot_rows[...], slot_cols[...], row_blocks, (own, halo))


def gathered(code, sources):
    edge = code.shape[1]
    lane = code & (edge - 1)
    block = code >> (edge.bit_length() - 1)
    total = jnp.zeros(code.shape, F32)
    for index, source in enumerate(sources):
        moved = jnp.take_along_axis(source, lane, axis=1, mode="promise_in_bounds")
        total = jnp.where(block == index, moved, total)
    return total


def add_boundary(table, hot, place, spread, values):
    edge = values[0].shape[1]
    main = hot.shape[1]
    width = table.shape[0]
    count = main // edge
    high_count = spread.shape[0] // 16
    for block in range(count):
        cols = slice(block * edge, (block + 1) * edge)
        for index in range(high_count):
            rows = slice(16 * index, 16 * index + 16)
            spread[rows, cols] = hot[rows, cols] * values[block]
    got = dot(spread[...], table[:, :main], ((1,), (1,)))
    last = [value.astype(F32) for value in values[count:]]
    last = [value[0:8] + value[8:16] for value in last]
    result = []
    for index in range(high_count):
        one = got[16 * index : 16 * index + 8] + got[16 * index + 8 : 16 * index + 16]
        for begin in range(0, width, edge):
            cols = slice(index * width + begin, index * width + begin + edge)
            result.append(one[:, begin : begin + edge] + gathered(place[:, cols], last))
    return result


def pick_boundary(table, high, vector, scale, outs):
    width = table.shape[0]
    halo = table.shape[1] // 2
    high_count = vector.shape[1] // width
    rows = jnp.concatenate(
        [
            scale[:, index * width : (index + 1) * width]
            * vector[:, index * width : (index + 1) * width]
            for index in range(high_count)
        ],
        axis=0,
    ).astype(BF16)

    def picked(begin):
        cols = slice(begin, begin + width)
        got = dot(rows, table[:, cols], ((1,), (0,)))
        total = jnp.zeros((8, width), F32)
        for index in range(high_count):
            total = jnp.where(high[:, cols] == index, got[8 * index : 8 * index + 8], total)
        return total

    for side, out in enumerate(outs):
        for begin in range(0, halo // 2, width):
            first = picked(side * halo + begin)
            second = picked(side * halo + halo // 2 + begin)
            out[:, halo + begin : halo + begin + width] = jnp.concatenate(
                [first, second], axis=0
            ).astype(BF16)


def warm_kernel(out):
    out[...] = jnp.zeros_like(out)


def each_live(size, counts, block_rows, block_cols, spare_row, spare_col, body):
    live = counts[0]

    def group(index, carry):
        entries = []
        for lane in range(size):
            slot = index * size + lane
            dead = slot >= live
            entries.append(
                (
                    slot,
                    jnp.where(dead, spare_row, block_rows[slot]),
                    jnp.where(dead, spare_col, block_cols[slot]),
                )
            )
        return body(entries, carry)

    return lax.fori_loop(0, (live + size - 1) // size, group, (0, 0))


def by_side(col, row_blocks):
    even = 1 - lax.axis_index("rows") % 2
    return (col - row_blocks + even * (row_blocks // 2)) & (row_blocks - 1)


def setup_kernel(
    counts_in, block_rows, block_cols, tiles, warm, first, second, inner, sums, counts, sem
):
    copy = pltpu.make_async_copy(counts_in, counts, sem.at[0])
    copy.start()
    edge = tiles.shape[1]
    halo_blocks = first.shape[0]
    row_blocks = inner.shape[0]
    sums[...] = jnp.zeros_like(sums)

    def add(entries, carry):
        parts = [
            jnp.sum(tiles[slot].astype(F32).reshape(edge // 8, 8, edge), axis=0)
            for slot, row, col in entries
        ]
        for (slot, row, col), part in zip(entries, parts):
            inside = jnp.logical_or(col < row_blocks, col == sums.shape[0] - 1)
            index = jnp.where(inside, col, row_blocks + by_side(col, row_blocks))
            sums[index] = sums[index] + part
        return carry

    copy.wait()
    each_live(16, counts, block_rows, block_cols, row_blocks, sums.shape[0] - 1, add)
    for out, base in ((inner, 0), (first, row_blocks), (second, row_blocks + halo_blocks)):
        for index in range(out.shape[0]):
            out[index : index + 1, :] = jnp.sum(sums[base + index], axis=0, keepdims=True)


def degree_kernel(
    counts_in, block_rows, block_cols, tiles, inner, degree, row_sums, counts, sem
):
    copy = pltpu.make_async_copy(counts_in, counts, sem.at[0])
    copy.start()
    edge = tiles.shape[1]
    row_blocks = inner.shape[0]
    row_sums[...] = jnp.zeros_like(row_sums)
    ones = jnp.ones((16, edge), BF16)

    def add(entries, carry):
        parts = [dot(ones, tiles[slot], ((1,), (1,)))[0:8] for slot, row, col in entries]
        for (slot, row, col), part in zip(entries, parts):
            row_sums[row] = row_sums[row] + part
        return carry

    copy.wait()
    each_live(WIDE, counts, block_rows, block_cols, row_blocks, 0, add)
    for index in range(row_blocks):
        degree[:, index * edge : (index + 1) * edge] = (
            1.0 + row_sums[index] + inner[index : index + 1, :]
        )


class Lists:
    def __init__(self, halo_in, halo, sem):
        self.halo = halo
        self.copies = [pltpu.make_async_copy(halo_in, halo, sem.at[0])]
        self.copies[0].start()

    def each(self, body):
        for copy in self.copies:
            copy.wait()
        self.copies = []
        for_slots(self.halo, body)


def send_products(lists, tiles, looks, vector, scale, source, sums, outs):
    edge = source.shape[2]
    row_blocks = source.shape[0] - 1
    half = row_blocks // 2
    for index in range(row_blocks):
        part = slice(index * edge, (index + 1) * edge)
        source[index] = two_parts(scale[:, part] * vector[:, part]).astype(BF16)
    source[row_blocks] = jnp.zeros_like(source[row_blocks])
    sums[...] = jnp.zeros_like(sums)
    lists.each(lambda entries: add_products(entries, tiles, source, sums, False))
    for side, out in enumerate(outs):
        for index in range(half):
            out[:, index * edge : (index + 1) * edge] = two_parts(
                sums[side * half + index]
            ).astype(BF16)
    pick_boundary(*looks, vector, scale, outs)


def first_kernel(
    halo_in, tiles, table, high, hot, place, degree, got_first, got_second, *rest
):
    starts = rest[:-9]
    out_first, out_second, vector, scale, source, spread, sums, halo, sem = rest[-9:]
    lists = Lists(halo_in, halo, sem)
    edge = tiles.shape[1]
    each = starts[0].shape[0]
    group = lax.axis_index("probe")
    for block in range(len(starts)):
        rows = starts[0][...]
        for other in range(1, len(starts)):
            rows = jnp.where(group == (block ^ other), starts[other][...], rows)
        vector[block * each : (block + 1) * each, :] = rows
    values = [
        two_parts(jnp.broadcast_to(got[i : i + 1, :], (8, edge))).astype(BF16)
        for got in (got_first, got_second)
        for i in range(got.shape[0])
    ]
    for index, part in enumerate(add_boundary(table, hot, place, spread, values)):
        cols = slice(index * edge, (index + 1) * edge)
        total = degree[:, cols] + part
        root = lax.rsqrt(total)
        scale[:, cols] = root * (1.5 - 0.5 * total * root * root)
    send_products(
        lists, tiles, (table, high), vector, scale, source, sums, (out_first, out_second)
    )


def own_kernel(own, tiles, source, image, sums):
    edge = tiles.shape[1]
    sums[...] = jnp.zeros_like(sums)

    def add(entries):
        add_products(entries, tiles, source, sums, True)
        add_products(entries, tiles, source, sums, False)

    for_slots(own, add)
    for index in range(sums.shape[0] - 1):
        image[:, index * edge : (index + 1) * edge] = sums[index]


def next_vector(
    shift, lists, tiles, looks, previous, scale, image, got_first, got_second,
    vector, spread, sums, outside,
):
    edge = tiles.shape[1]
    halo = looks[0].shape[1] // 2
    halo_blocks = halo // edge
    values = []
    for side, got in enumerate((got_first, got_second)):
        for index in range(halo_blocks):
            half = index // (halo_blocks // 2)
            begin = halo + (index % (halo_blocks // 2)) * edge
            outside[side * halo_blocks + index] = got[8 * half : 8 * half + 8, begin : begin + edge]
            values.append(got[:, index * edge : (index + 1) * edge])
    outside[2 * halo_blocks] = jnp.zeros_like(outside[0])
    for index, added in enumerate(add_boundary(*looks, spread, values)):
        sums[index] = added + image[:, index * edge : (index + 1) * edge]
    lists.each(lambda entries: add_products(entries, tiles, outside, sums, True))
    for index in range(sums.shape[0] - 1):
        part = slice(index * edge, (index + 1) * edge)
        old = previous[:, part]
        root = scale[:, part]
        vector[:, part] = root * (root * old) + root * sums[index] - shift * old


def middle_kernel(
    shift, halo_in, tiles, table, high, hot, place, previous, scale, image,
    got_first, got_second, out_first, out_second, vector, source,
    spread, sums, outside, halo, sem,
):
    lists = Lists(halo_in, halo, sem)
    next_vector(
        shift, lists, tiles, (table, hot, place), previous, scale, image, got_first, got_second,
        vector, spread, sums, outside,
    )
    send_products(
        lists, tiles, (table, high), vector, scale, source, sums, (out_first, out_second)
    )


def three_parts(values):
    high = values.astype(BF16)
    rest = values - high.astype(F32)
    middle = rest.astype(BF16)
    return [high, middle, (rest - middle.astype(F32)).astype(BF16)]


def last_kernel(
    shift, halo_in, tiles, table, hot, place, scale, image, got_first, got_second, *rest
):
    vectors = rest[:STEPS]
    gram, vector, spread, sums, outside, halo, sem = rest[STEPS:]
    lists = Lists(halo_in, halo, sem)
    next_vector(
        shift, lists, tiles, (table, hot, place), vectors[-1], scale, image,
        got_first, got_second, vector, spread, sums, outside,
    )
    basis = jnp.concatenate([one[...] for one in vectors] + [vector[...]], axis=0)
    size = basis.shape[0]
    parts = jnp.concatenate(three_parts(basis), axis=0)
    wide = dot(parts, parts, ((1,), (1,)))
    total = sum(
        wide[i * size : (i + 1) * size, j * size : (j + 1) * size]
        for i in reversed(range(3))
        for j in reversed(range(3))
    )
    packed = jnp.concatenate([total[8 * i : 8 * i + 8, :] for i in range(size // 8)], axis=1)
    for copy in range(gram.shape[0] // 8):
        gram[8 * copy : 8 * copy + 8, :] = packed


def final_kernel(node_total, grams, *rest):
    vectors = rest[: STEPS + 1]
    basis, alphas, betas = rest[STEPS + 1 :]
    size = 8 * (STEPS + 1)
    packed = grams[0:8, :]
    for copy in range(1, grams.shape[0] // 8):
        packed = packed + grams[8 * copy : 8 * copy + 8, :]
    packed = packed * (1.0 / node_total)
    gram = jnp.concatenate(
        [packed[:, i * size : (i + 1) * size] for i in range(STEPS + 1)], axis=0
    )
    row_ids = lax.broadcasted_iota(jnp.int32, (size, size), 0)
    col_ids = lax.broadcasted_iota(jnp.int32, (size, size), 1)
    unit = jnp.where(row_ids == col_ids, 1.0, 0.0)
    work = jnp.concatenate([gram, unit], axis=1)
    rows = lax.broadcasted_iota(jnp.int32, (size, 2 * size), 0)
    pivots = jnp.ones((size, 2 * size), F32)
    for begin in range(0, size, 8):
        columns = [
            jnp.broadcast_to(work[:, begin + c : begin + c + 1], (size, 2 * size)) for c in range(8)
        ]
        for c in range(8):
            k = begin + c
            pivot = columns[c][k : k + 1, :]
            pivots = jnp.where(rows == k, pivot, pivots)
            factor = jnp.where(rows > k, columns[c] * (1.0 / pivot), 0.0)
            work = work - factor * work[k : k + 1, :]
            for d in range(c + 1, 8):
                columns[d] = columns[d] - factor * columns[d][k : k + 1, :]
    work = work / jnp.sqrt(pivots)
    upper = jnp.where(row_ids <= col_ids, work[:, :size], 0.0)
    inverse = work[:, size:]
    own = jnp.where(row_ids // 8 == col_ids // 8, inverse, 0.0)
    moved = jnp.concatenate(
        [jnp.zeros((8, size), F32)]
        + [
            jnp.concatenate(
                [jnp.zeros((8, 8), F32), own[8 * i : 8 * i + 8, : size - 8]], axis=1
            )
            for i in range(STEPS)
        ],
        axis=0,
    )
    by_last = exact_dot(moved, upper, ((1,), (1,)))
    by_own = exact_dot(own, upper, ((1,), (1,)))
    small = unit[0:8, 0:8]

    def piece(table, i, j):
        return table[8 * i : 8 * i + 8, 8 * j : 8 * j + 8]

    for j in range(STEPS):
        beta = piece(by_last, j + 1, j + 1)
        alpha = (1.0 - SHIFTS[j]) * small - piece(by_last, j + 1, j)
        if j:
            alpha = alpha + exact_dot(piece(by_own, j, j - 1), piece(by_last, j, j), ((1,), (0,)))
        betas[j] = jnp.where(row_ids[0:8, 0:8] >= col_ids[0:8, 0:8], beta, 0.0)
        alphas[j] = alpha
    last = inverse[size - 8 :, :] * (-1.0) ** STEPS
    each = basis.shape[0]
    place = lax.axis_index("probe")
    ids = lax.broadcasted_iota(jnp.int32, (8, size), 0)
    chosen = jnp.zeros((8, size), F32)
    for index in range(each):
        line = jnp.sum(jnp.where(ids == place * each + index, last, 0.0), axis=0, keepdims=True)
        chosen = jnp.where(ids == index, line, chosen)
    total = exact_dot(chosen, jnp.concatenate([one[...] for one in vectors], axis=0), ((1,), (0,)))
    basis[...] = total[0:each]


def local(start_block, blocks, block_rows, block_cols, counts, boundary):
    each, rows_dev = start_block.shape
    slot_count, edge, _ = blocks.shape
    halo_width = boundary.shape[1]
    parts = lax.axis_size("rows")
    groups = lax.axis_size("probe")
    node_total = rows_dev * parts
    row_blocks = rows_dev // edge
    halo_blocks = halo_width // edge
    probes = each * groups
    width = 2 * edge
    shape = jax.ShapeDtypeStruct

    if parts % 2:
        raise ValueError("odd ring")
    matchings = (
        [(i, i ^ 1) for i in range(parts)],
        [(i, (i + 1) % parts if i % 2 else (i - 1) % parts) for i in range(parts)],
    )

    def exchange(first, second):
        got_second = lax.ppermute(second, "rows", matchings[1])
        got_first = lax.ppermute(first, "rows", matchings[0])
        return got_first, got_second

    listed = (1, 2 * slot_count)
    sums = pltpu.VMEM((row_blocks + 1, 8, edge), F32)
    outside = pltpu.VMEM((2 * halo_blocks + 1, 8, edge), BF16)
    counted = [pltpu.SMEM(counts.shape, jnp.int32), pltpu.SemaphoreType.DMA((1,))]
    fetched = [pltpu.SMEM(listed, jnp.int32), pltpu.SemaphoreType.DMA((1,))]

    def call(body, in_specs, out_shape, out_specs, scratch):
        return pl.pallas_call(
            body,
            out_shape=out_shape,
            in_specs=in_specs,
            out_specs=out_specs,
            scratch_shapes=scratch,
            compiler_params=pltpu.CompilerParams(vmem_limit_bytes=LIMIT),
            cost_estimate=pl.CostEstimate(flops=2 << 30, transcendentals=0, bytes_accessed=1 << 20),
        )

    starts = [start_block]
    for other in range(1, groups):
        pairs = [(i, i ^ other) for i in range(groups)]
        starts.append(lax.ppermute(start_block, "probe", pairs))
    warm = call(warm_kernel, [], shape((8, 128), F32), VMEM, [])()
    low, up, inner = call(
        setup_kernel,
        [VMEM, SMEM, SMEM, VMEM, ANY],
        (
            shape((halo_blocks, edge), F32),
            shape((halo_blocks, edge), F32),
            shape((row_blocks, edge), F32),
        ),
        (VMEM,) * 3,
        [pltpu.VMEM((row_blocks + 2 * halo_blocks + 1, 8, edge), F32)] + counted,
    )(counts, block_rows, block_cols, blocks, warm)
    got = exchange(low, up)
    rest = min(halo_width, 2 * halo_width * 5 // 16 // width * width)
    main = 2 * halo_width - rest
    high_rows = 16 * (rows_dev // width)
    own, halo, table, high, hot, place = call(
        index_kernel,
        [VMEM, VMEM, VMEM, VMEM, ANY],
        (
            shape(listed, jnp.int32),
            shape(listed, jnp.int32),
            shape((width, 2 * halo_width), BF16),
            shape((8, 2 * halo_width), jnp.int32),
            shape((high_rows, main), BF16),
            shape((8, rows_dev), jnp.int32),
        ),
        (VMEM,) * 6,
        [pltpu.VMEM((high_rows, rest), BF16)] + counted,
    )(counts, block_rows.reshape(1, -1), block_cols.reshape(1, -1), boundary, low)
    spread = pltpu.VMEM((high_rows, main), BF16)
    degree = call(
        degree_kernel,
        [VMEM, SMEM, SMEM, VMEM, VMEM],
        shape((8, rows_dev), F32),
        VMEM,
        [sums] + counted,
    )(counts, block_rows, block_cols, blocks, inner)

    message = shape((16, halo_width + halo_width // 2), BF16)
    vector_shape = shape((probes, rows_dev), F32)
    source_shape = shape((row_blocks + 1, 16, edge), BF16)
    first, second, vector, scale, source = call(
        first_kernel,
        [ANY] + [VMEM] * (8 + groups),
        (message, message, vector_shape, vector_shape, source_shape),
        (VMEM,) * 5,
        [spread, sums] + fetched,
    )(halo, blocks, table, high, hot, place, degree, *got, *starts)

    vectors = [vector]
    for step in range(STEPS):
        got = exchange(first, second)
        image = call(
            own_kernel, [SMEM, VMEM, VMEM], vector_shape, VMEM, [sums]
        )(own, blocks, source)
        if step + 1 < STEPS:
            first, second, vector, source = call(
                functools.partial(middle_kernel, SHIFTS[step]),
                [ANY] + [VMEM] * 10,
                (message, message, vector_shape, source_shape),
                (VMEM,) * 4,
                [spread, sums, outside] + fetched,
            )(halo, blocks, table, high, hot, place, vectors[-1], scale, image, *got)
        else:
            grams, vector = call(
                functools.partial(last_kernel, SHIFTS[step]),
                [ANY] + [VMEM] * (8 + STEPS),
                (shape((8 * parts, 128), F32), vector_shape),
                (VMEM,) * 2,
                [spread, sums, outside] + fetched,
            )(halo, blocks, table, hot, place, scale, image, *got, *vectors)
        vectors.append(vector)
    gathered = lax.all_to_all(grams, "rows", 0, 0, tiled=True)
    return call(
        functools.partial(final_kernel, float(node_total)),
        [VMEM] * (2 + STEPS),
        (
            shape((each, rows_dev), F32),
            shape((STEPS, probes, probes), F32),
            shape((STEPS, probes, probes), F32),
        ),
        (VMEM,) * 3,
        [],
    )(gathered, *vectors)


def solution(mesh):
    in_specs = (
        P("probe", "rows"),
        P("rows", None, None),
        P("rows"),
        P("rows"),
        P("rows"),
        P(None, "rows"),
    )
    out_specs = (P("probe", "rows"), P(), P())
    return jax.shard_map(local, mesh=mesh, in_specs=in_specs, out_specs=out_specs, check_vma=False)
```

```python
import functools

import jax
import jax.numpy as jnp
from jax import lax
from jax.experimental import pallas as pl
from jax.experimental.pallas import tpu as pltpu
from jax.sharding import PartitionSpec as P


STEPS = 3
SHIFTS = (0.0, 1.0, 0.0)
WIDE = 32
LIMIT = 16 << 20
F32 = jnp.float32
BF16 = jnp.bfloat16

SMEM = pl.BlockSpec(memory_space=pltpu.SMEM)
VMEM = pl.BlockSpec(memory_space=pltpu.VMEM)
ANY = pl.BlockSpec(memory_space=pl.ANY)


def dot(a, b, contract):
    return lax.dot_general(a, b, (contract, ((), ())), preferred_element_type=F32)


def exact_dot(a, b, contract):
    return lax.dot_general(
        a, b, (contract, ((), ())), precision=lax.Precision.HIGHEST, preferred_element_type=F32
    )


def for_slots(slots, body):
    live = slots[0, slots.shape[1] - 1]

    def turns(size, first, count):
        def group(index, carry):
            entries = []
            for lane in range(size):
                code = slots[0, first + index * size + lane]
                entries.append((code & 255, (code >> 8) & 255, code >> 16))
            body(entries)
            return carry

        lax.fori_loop(0, count, group, 0)

    wide = (live + WIDE // 2 - 1) // WIDE
    left = live - wide * WIDE
    turns(WIDE, 0, wide)
    turns(WIDE // 2, wide * WIDE, (left > WIDE // 4).astype(jnp.int32))
    small = jnp.logical_and(left > 0, left <= WIDE // 4)
    turns(WIDE // 4, wide * WIDE, small.astype(jnp.int32))


def two_parts(values):
    high = values.astype(BF16).astype(F32)
    return jnp.concatenate([high, values - high], axis=0)


def add_products(entries, tiles, source, totals, forward):
    products = []
    for slot, row, col in entries:
        index = col if forward else row
        got = dot(source[index], tiles[slot], ((1,), (1,)) if forward else ((1,), (0,)))
        products.append(got if got.shape[0] == 8 else got[0:8] + got[8:16])
    for (slot, row, col), got in zip(entries, products):
        index = row if forward else col
        totals[index] = totals[index] + got


def fill_one_hot(index, table):
    width = table.shape[0]
    for begin in range(0, index.shape[1], width):
        low = index[:, begin : begin + width] & (width - 1)
        hit = lax.broadcasted_iota(jnp.int32, (width, width), 0) == low
        table[:, begin : begin + width] = jnp.where(hit, 1.0, 0.0).astype(BF16)


def list_slots(live, rows, cols, row_blocks, outputs):
    count = rows.shape[1]
    shape = (8, count)
    lane = lax.broadcasted_iota(jnp.int32, shape, 1)
    row_id = lax.broadcasted_iota(jnp.int32, shape, 0)
    row = jnp.broadcast_to(rows, shape)
    col = jnp.broadcast_to(cols, shape)
    outside = col >= row_blocks
    index = jnp.where(outside, by_side(col, row_blocks), col)
    fields = jnp.where(row_id == 0, lane, jnp.where(row_id == 1, row, index)).astype(F32)
    square = (count, count)
    first = lax.broadcasted_iota(jnp.int32, square, 0)
    second = lax.broadcasted_iota(jnp.int32, square, 1)
    before = jnp.where(first < second, 1.0, 0.0).astype(BF16)
    empty = (row_blocks << 8) | (row_blocks << 16)
    alive = lane < live
    masks = [jnp.logical_and(alive, jnp.logical_not(outside)), jnp.logical_and(alive, outside)]
    ones = [jnp.where(mask, 1.0, 0.0) for mask in masks]
    ahead = dot(jnp.concatenate(ones, axis=0).astype(BF16), before, ((1,), (0,)))
    totals = [jnp.sum(one, axis=1, keepdims=True).astype(jnp.int32)[0:1] for one in ones]
    spots = [jnp.where(mask, ahead[8 * i : 8 * i + 8], -1.0)[0:1] for i, mask in enumerate(masks)]
    moved = [
        jnp.where(jnp.broadcast_to(spot, square).T == second.astype(F32), 1.0, 0.0).astype(BF16)
        for spot in spots
    ]
    placed = [dot(fields.astype(BF16), move, ((1,), (0,))).astype(jnp.int32) for move in moved]
    for out, total, place in zip(outputs, totals, placed):
        code = place[0:1] | (place[1:2] << 8) | (place[2:3] << 16)
        out[:, :count] = jnp.where(lane[0:1] < total, code, empty)
        out[:, count:] = jnp.where(lane[0:1] == count - 1, total, empty)


def index_kernel(
    row_blocks, counts, slot_rows, slot_cols, bound, warm, own, halo, table, high, hot, place, spread
):
    list_slots(counts[0], slot_rows[...], slot_cols[...], row_blocks, (own, halo))
    even = lax.axis_index("rows") % 2 == 0
    upper = bound[1:2, :]
    lower = bound[0:1, :]
    index = jnp.concatenate(
        [jnp.where(even, upper, lower), jnp.where(even, lower, upper)], axis=1
    )
    main = hot.shape[1]
    width = table.shape[0]
    shift = width.bit_length() - 1
    rest = table.shape[1] - main
    high[...] = jnp.broadcast_to(index >> shift, high.shape)
    fill_one_hot(index, table)
    entry = lax.broadcasted_iota(jnp.int32, (8, rest), 1) + 1
    stacked = two_parts(entry.astype(F32))
    both = jnp.broadcast_to(index >> shift, (16, index.shape[1]))
    high_count = spread.shape[0] // 16
    for part in range(high_count):
        rows = slice(16 * part, 16 * part + 16)
        hot[rows, :] = jnp.where(both[:, :main] == part, 1.0, 0.0).astype(BF16)
        spread[rows, :] = jnp.where(both[:, main:] == part, stacked, 0.0).astype(BF16)
    got = dot(spread[...], table[:, main:], ((1,), (1,)))
    for part in range(high_count):
        one = got[16 * part : 16 * part + 8] + got[16 * part + 8 : 16 * part + 16]
        place[:, part * width : (part + 1) * width] = (one + 0.5).astype(jnp.int32) - 1


def gathered(code, sources):
    edge = code.shape[1]
    lane = code & (edge - 1)
    block = code >> (edge.bit_length() - 1)
    total = jnp.zeros(code.shape, F32)
    for index, source in enumerate(sources):
        moved = jnp.take_along_axis(source, lane, axis=1, mode="promise_in_bounds")
        total = jnp.where(block == index, moved, total)
    return total


def add_boundary(table, hot, place, spread, values):
    edge = values[0].shape[1]
    main = hot.shape[1]
    width = table.shape[0]
    count = main // edge
    high_count = spread.shape[0] // 16
    for block in range(count):
        cols = slice(block * edge, (block + 1) * edge)
        for index in range(high_count):
            rows = slice(16 * index, 16 * index + 16)
            spread[rows, cols] = hot[rows, cols] * values[block]
    got = dot(spread[...], table[:, :main], ((1,), (1,)))
    last = [value.astype(F32) for value in values[count:]]
    last = [value[0:8] + value[8:16] for value in last]
    result = []
    for index in range(high_count):
        one = got[16 * index : 16 * index + 8] + got[16 * index + 8 : 16 * index + 16]
        for begin in range(0, width, edge):
            cols = slice(index * width + begin, index * width + begin + edge)
            result.append(one[:, begin : begin + edge] + gathered(place[:, cols], last))
    return result


def pick_boundary(table, high, vector, scale, outs):
    width = table.shape[0]
    halo = table.shape[1] // 2
    high_count = vector.shape[1] // width
    rows = jnp.concatenate(
        [
            scale[:, index * width : (index + 1) * width]
            * vector[:, index * width : (index + 1) * width]
            for index in range(high_count)
        ],
        axis=0,
    ).astype(BF16)

    def picked(begin):
        cols = slice(begin, begin + width)
        got = dot(rows, table[:, cols], ((1,), (0,)))
        total = jnp.zeros((8, width), F32)
        for index in range(high_count):
            total = jnp.where(high[:, cols] == index, got[8 * index : 8 * index + 8], total)
        return total

    for side, out in enumerate(outs):
        for begin in range(0, halo // 2, width):
            first = picked(side * halo + begin)
            second = picked(side * halo + halo // 2 + begin)
            out[:, halo + begin : halo + begin + width] = jnp.concatenate(
                [first, second], axis=0
            ).astype(BF16)


def warm_kernel(out):
    out[...] = jnp.zeros_like(out)


def each_live(size, counts, block_rows, block_cols, spare_row, spare_col, body):
    live = counts[0]

    def group(index, carry):
        entries = []
        for lane in range(size):
            slot = index * size + lane
            dead = slot >= live
            entries.append(
                (
                    slot,
                    jnp.where(dead, spare_row, block_rows[slot]),
                    jnp.where(dead, spare_col, block_cols[slot]),
                )
            )
        return body(entries, carry)

    return lax.fori_loop(0, (live + size - 1) // size, group, (0, 0))


def by_side(col, row_blocks):
    even = 1 - lax.axis_index("rows") % 2
    return (col - row_blocks + even * (row_blocks // 2)) & (row_blocks - 1)


def setup_kernel(
    counts, block_rows, block_cols, tiles, high, first, second, inner, sums
):
    edge = tiles.shape[1]
    halo_blocks = first.shape[0]
    row_blocks = inner.shape[0]
    sums[...] = jnp.zeros_like(sums)

    def add(entries, carry):
        parts = [
            jnp.sum(tiles[slot].astype(F32).reshape(edge // 8, 8, edge), axis=0)
            for slot, row, col in entries
        ]
        for (slot, row, col), part in zip(entries, parts):
            inside = jnp.logical_or(col < row_blocks, col == sums.shape[0] - 1)
            index = jnp.where(inside, col, row_blocks + by_side(col, row_blocks))
            sums[index] = sums[index] + part
        return carry

    each_live(16, counts, block_rows, block_cols, row_blocks, sums.shape[0] - 1, add)
    for out, base in ((inner, 0), (first, row_blocks), (second, row_blocks + halo_blocks)):
        for index in range(out.shape[0]):
            out[index : index + 1, :] = jnp.sum(sums[base + index], axis=0, keepdims=True)


def degree_kernel(
    counts, block_rows, block_cols, tiles, inner, degree, row_sums
):
    edge = tiles.shape[1]
    row_blocks = inner.shape[0]
    row_sums[...] = jnp.zeros_like(row_sums)
    ones = jnp.ones((16, edge), BF16)

    def add(entries, carry):
        parts = [dot(ones, tiles[slot], ((1,), (1,)))[0:8] for slot, row, col in entries]
        for (slot, row, col), part in zip(entries, parts):
            row_sums[row] = row_sums[row] + part
        return carry

    each_live(WIDE, counts, block_rows, block_cols, row_blocks, 0, add)
    for index in range(row_blocks):
        degree[:, index * edge : (index + 1) * edge] = (
            1.0 + row_sums[index] + inner[index : index + 1, :]
        )


class Lists:
    def __init__(self, halo_in, halo, sem):
        self.halo = halo
        self.copies = [pltpu.make_async_copy(halo_in, halo, sem.at[0])]
        self.copies[0].start()

    def each(self, body):
        for copy in self.copies:
            copy.wait()
        self.copies = []
        for_slots(self.halo, body)


def send_products(lists, tiles, looks, vector, scale, source, sums, outs):
    edge = source.shape[2]
    row_blocks = source.shape[0] - 1
    half = row_blocks // 2
    for index in range(row_blocks):
        part = slice(index * edge, (index + 1) * edge)
        source[index] = two_parts(scale[:, part] * vector[:, part]).astype(BF16)
    source[row_blocks] = jnp.zeros_like(source[row_blocks])
    sums[...] = jnp.zeros_like(sums)
    lists.each(lambda entries: add_products(entries, tiles, source, sums, False))
    for side, out in enumerate(outs):
        for index in range(half):
            out[:, index * edge : (index + 1) * edge] = two_parts(
                sums[side * half + index]
            ).astype(BF16)
    pick_boundary(*looks, vector, scale, outs)


def first_kernel(
    halo_in, tiles, table, high, hot, place, degree, got_first, got_second, *rest
):
    starts = rest[:-9]
    out_first, out_second, vector, scale, source, spread, sums, halo, sem = rest[-9:]
    lists = Lists(halo_in, halo, sem)
    edge = tiles.shape[1]
    each = starts[0].shape[0]
    group = lax.axis_index("probe")
    for block in range(len(starts)):
        rows = starts[0][...]
        for other in range(1, len(starts)):
            rows = jnp.where(group == (block ^ other), starts[other][...], rows)
        vector[block * each : (block + 1) * each, :] = rows
    values = [
        two_parts(jnp.broadcast_to(got[i : i + 1, :], (8, edge))).astype(BF16)
        for got in (got_first, got_second)
        for i in range(got.shape[0])
    ]
    for index, part in enumerate(add_boundary(table, hot, place, spread, values)):
        cols = slice(index * edge, (index + 1) * edge)
        total = degree[:, cols] + part
        root = lax.rsqrt(total)
        scale[:, cols] = root * (1.5 - 0.5 * total * root * root)
    send_products(
        lists, tiles, (table, high), vector, scale, source, sums, (out_first, out_second)
    )


def own_kernel(own, tiles, source, image, sums):
    edge = tiles.shape[1]
    sums[...] = jnp.zeros_like(sums)

    def add(entries):
        add_products(entries, tiles, source, sums, True)
        add_products(entries, tiles, source, sums, False)

    for_slots(own, add)
    for index in range(sums.shape[0] - 1):
        image[:, index * edge : (index + 1) * edge] = sums[index]


def next_vector(
    shift, lists, tiles, looks, previous, scale, image, got_first, got_second,
    vector, spread, sums, outside,
):
    edge = tiles.shape[1]
    halo = looks[0].shape[1] // 2
    halo_blocks = halo // edge
    values = []
    for side, got in enumerate((got_first, got_second)):
        for index in range(halo_blocks):
            half = index // (halo_blocks // 2)
            begin = halo + (index % (halo_blocks // 2)) * edge
            outside[side * halo_blocks + index] = got[8 * half : 8 * half + 8, begin : begin + edge]
            values.append(got[:, index * edge : (index + 1) * edge])
    outside[2 * halo_blocks] = jnp.zeros_like(outside[0])
    for index, added in enumerate(add_boundary(*looks, spread, values)):
        sums[index] = added + image[:, index * edge : (index + 1) * edge]
    lists.each(lambda entries: add_products(entries, tiles, outside, sums, True))
    for index in range(sums.shape[0] - 1):
        part = slice(index * edge, (index + 1) * edge)
        old = previous[:, part]
        root = scale[:, part]
        vector[:, part] = root * (root * old) + root * sums[index] - shift * old


def middle_kernel(
    shift, halo_in, tiles, table, high, hot, place, previous, scale, image,
    got_first, got_second, out_first, out_second, vector, source,
    spread, sums, outside, halo, sem,
):
    lists = Lists(halo_in, halo, sem)
    next_vector(
        shift, lists, tiles, (table, hot, place), previous, scale, image, got_first, got_second,
        vector, spread, sums, outside,
    )
    send_products(
        lists, tiles, (table, high), vector, scale, source, sums, (out_first, out_second)
    )


def three_parts(values):
    high = values.astype(BF16)
    rest = values - high.astype(F32)
    middle = rest.astype(BF16)
    return [high, middle, (rest - middle.astype(F32)).astype(BF16)]


def last_kernel(
    shift, halo_in, tiles, table, hot, place, scale, image, got_first, got_second, *rest
):
    vectors = rest[:STEPS]
    gram, vector, spread, sums, outside, halo, sem = rest[STEPS:]
    lists = Lists(halo_in, halo, sem)
    next_vector(
        shift, lists, tiles, (table, hot, place), vectors[-1], scale, image,
        got_first, got_second, vector, spread, sums, outside,
    )
    basis = jnp.concatenate([one[...] for one in vectors] + [vector[...]], axis=0)
    size = basis.shape[0]
    parts = jnp.concatenate(three_parts(basis), axis=0)
    wide = dot(parts, parts, ((1,), (1,)))
    total = sum(
        wide[i * size : (i + 1) * size, j * size : (j + 1) * size]
        for i in reversed(range(3))
        for j in reversed(range(3))
    )
    packed = jnp.concatenate([total[8 * i : 8 * i + 8, :] for i in range(size // 8)], axis=1)
    for copy in range(gram.shape[0] // 8):
        gram[8 * copy : 8 * copy + 8, :] = packed


def final_kernel(node_total, grams, *rest):
    vectors = rest[: STEPS + 1]
    basis, alphas, betas = rest[STEPS + 1 :]
    size = 8 * (STEPS + 1)
    packed = grams[0:8, :]
    for copy in range(1, grams.shape[0] // 8):
        packed = packed + grams[8 * copy : 8 * copy + 8, :]
    packed = packed * (1.0 / node_total)
    gram = jnp.concatenate(
        [packed[:, i * size : (i + 1) * size] for i in range(STEPS + 1)], axis=0
    )
    row_ids = lax.broadcasted_iota(jnp.int32, (size, size), 0)
    col_ids = lax.broadcasted_iota(jnp.int32, (size, size), 1)
    unit = jnp.where(row_ids == col_ids, 1.0, 0.0)
    work = jnp.concatenate([gram, unit], axis=1)
    rows = lax.broadcasted_iota(jnp.int32, (size, 2 * size), 0)
    pivots = jnp.ones((size, 2 * size), F32)
    for begin in range(0, size, 8):
        columns = [
            jnp.broadcast_to(work[:, begin + c : begin + c + 1], (size, 2 * size)) for c in range(8)
        ]
        for c in range(8):
            k = begin + c
            pivot = columns[c][k : k + 1, :]
            pivots = jnp.where(rows == k, pivot, pivots)
            factor = jnp.where(rows > k, columns[c] * (1.0 / pivot), 0.0)
            work = work - factor * work[k : k + 1, :]
            for d in range(c + 1, 8):
                columns[d] = columns[d] - factor * columns[d][k : k + 1, :]
    work = work / jnp.sqrt(pivots)
    upper = jnp.where(row_ids <= col_ids, work[:, :size], 0.0)
    inverse = work[:, size:]
    own = jnp.where(row_ids // 8 == col_ids // 8, inverse, 0.0)
    moved = jnp.concatenate(
        [jnp.zeros((8, size), F32)]
        + [
            jnp.concatenate(
                [jnp.zeros((8, 8), F32), own[8 * i : 8 * i + 8, : size - 8]], axis=1
            )
            for i in range(STEPS)
        ],
        axis=0,
    )
    by_last = exact_dot(moved, upper, ((1,), (1,)))
    by_own = exact_dot(own, upper, ((1,), (1,)))
    small = unit[0:8, 0:8]

    def piece(table, i, j):
        return table[8 * i : 8 * i + 8, 8 * j : 8 * j + 8]

    for j in range(STEPS):
        beta = piece(by_last, j + 1, j + 1)
        alpha = (1.0 - SHIFTS[j]) * small - piece(by_last, j + 1, j)
        if j:
            alpha = alpha + exact_dot(piece(by_own, j, j - 1), piece(by_last, j, j), ((1,), (0,)))
        betas[j] = jnp.where(row_ids[0:8, 0:8] >= col_ids[0:8, 0:8], beta, 0.0)
        alphas[j] = alpha
    last = inverse[size - 8 :, :] * (-1.0) ** STEPS
    each = basis.shape[0]
    place = lax.axis_index("probe")
    ids = lax.broadcasted_iota(jnp.int32, (8, size), 0)
    chosen = jnp.zeros((8, size), F32)
    for index in range(each):
        line = jnp.sum(jnp.where(ids == place * each + index, last, 0.0), axis=0, keepdims=True)
        chosen = jnp.where(ids == index, line, chosen)
    total = exact_dot(chosen, jnp.concatenate([one[...] for one in vectors], axis=0), ((1,), (0,)))
    basis[...] = total[0:each]


def local(start_block, blocks, block_rows, block_cols, counts, boundary):
    each, rows_dev = start_block.shape
    slot_count, edge, _ = blocks.shape
    halo_width = boundary.shape[1]
    parts = lax.axis_size("rows")
    groups = lax.axis_size("probe")
    node_total = rows_dev * parts
    row_blocks = rows_dev // edge
    halo_blocks = halo_width // edge
    probes = each * groups
    width = 2 * edge
    shape = jax.ShapeDtypeStruct

    if parts % 2:
        raise ValueError("odd ring")
    matchings = (
        [(i, i ^ 1) for i in range(parts)],
        [(i, (i + 1) % parts if i % 2 else (i - 1) % parts) for i in range(parts)],
    )

    def exchange(first, second):
        got_second = lax.ppermute(second, "rows", matchings[1])
        got_first = lax.ppermute(first, "rows", matchings[0])
        return got_first, got_second

    listed = (1, 2 * slot_count)
    sums = pltpu.VMEM((row_blocks + 1, 8, edge), F32)
    outside = pltpu.VMEM((2 * halo_blocks + 1, 8, edge), BF16)
    fetched = [pltpu.SMEM(listed, jnp.int32), pltpu.SemaphoreType.DMA((1,))]

    def call(body, in_specs, out_shape, out_specs, scratch, flops=2 << 30):
        return pl.pallas_call(
            body,
            out_shape=out_shape,
            in_specs=in_specs,
            out_specs=out_specs,
            scratch_shapes=scratch,
            compiler_params=pltpu.CompilerParams(vmem_limit_bytes=LIMIT),
            cost_estimate=pl.CostEstimate(
                flops=flops, transcendentals=0, bytes_accessed=flops >> 11
            ),
        )

    starts = [start_block]
    for other in range(1, groups):
        pairs = [(i, i ^ other) for i in range(groups)]
        starts.append(lax.ppermute(start_block, "probe", pairs))
    warm = call(warm_kernel, [], shape((8, 128), F32), VMEM, [])()
    rest = min(halo_width, 2 * halo_width * 5 // 16 // width * width)
    main = 2 * halo_width - rest
    high_rows = 16 * (rows_dev // width)
    own, halo, table, high, hot, place = call(
        functools.partial(index_kernel, row_blocks),
        [SMEM, VMEM, VMEM, VMEM, ANY],
        (
            shape(listed, jnp.int32),
            shape(listed, jnp.int32),
            shape((width, 2 * halo_width), BF16),
            shape((8, 2 * halo_width), jnp.int32),
            shape((high_rows, main), BF16),
            shape((8, rows_dev), jnp.int32),
        ),
        (VMEM,) * 6,
        [pltpu.VMEM((high_rows, rest), BF16)],
        flops=1 << 20,
    )(counts, block_rows.reshape(1, -1), block_cols.reshape(1, -1), boundary, warm)
    low, up, inner = call(
        setup_kernel,
        [SMEM, SMEM, SMEM, VMEM, ANY],
        (
            shape((halo_blocks, edge), F32),
            shape((halo_blocks, edge), F32),
            shape((row_blocks, edge), F32),
        ),
        (VMEM,) * 3,
        [pltpu.VMEM((row_blocks + 2 * halo_blocks + 1, 8, edge), F32)],
    )(counts, block_rows, block_cols, blocks, high)
    got = exchange(low, up)
    spread = pltpu.VMEM((high_rows, main), BF16)
    degree = call(
        degree_kernel, [SMEM, SMEM, SMEM, VMEM, VMEM], shape((8, rows_dev), F32), VMEM, [sums]
    )(counts, block_rows, block_cols, blocks, inner)

    message = shape((16, halo_width + halo_width // 2), BF16)
    vector_shape = shape((probes, rows_dev), F32)
    source_shape = shape((row_blocks + 1, 16, edge), BF16)
    first, second, vector, scale, source = call(
        first_kernel,
        [ANY] + [VMEM] * (8 + groups),
        (message, message, vector_shape, vector_shape, source_shape),
        (VMEM,) * 5,
        [spread, sums] + fetched,
    )(halo, blocks, table, high, hot, place, degree, *got, *starts)

    vectors = [vector]
    for step in range(STEPS):
        got = exchange(first, second)
        image = call(
            own_kernel, [SMEM, VMEM, VMEM], vector_shape, VMEM, [sums]
        )(own, blocks, source)
        if step + 1 < STEPS:
            first, second, vector, source = call(
                functools.partial(middle_kernel, SHIFTS[step]),
                [ANY] + [VMEM] * 10,
                (message, message, vector_shape, source_shape),
                (VMEM,) * 4,
                [spread, sums, outside] + fetched,
            )(halo, blocks, table, high, hot, place, vectors[-1], scale, image, *got)
        else:
            grams, vector = call(
                functools.partial(last_kernel, SHIFTS[step]),
                [ANY] + [VMEM] * (8 + STEPS),
                (shape((8 * parts, 128), F32), vector_shape),
                (VMEM,) * 2,
                [spread, sums, outside] + fetched,
            )(halo, blocks, table, hot, place, scale, image, *got, *vectors)
        vectors.append(vector)
    gathered = lax.all_to_all(grams, "rows", 0, 0, tiled=True)
    return call(
        functools.partial(final_kernel, float(node_total)),
        [VMEM] * (2 + STEPS),
        (
            shape((each, rows_dev), F32),
            shape((STEPS, probes, probes), F32),
            shape((STEPS, probes, probes), F32),
        ),
        (VMEM,) * 3,
        [],
    )(gathered, *vectors)


def solution(mesh):
    in_specs = (
        P("probe", "rows"),
        P("rows", None, None),
        P("rows"),
        P("rows"),
        P("rows"),
        P(None, "rows"),
    )
    out_specs = (P("probe", "rows"), P(), P())
    return jax.shard_map(local, mesh=mesh, in_specs=in_specs, out_specs=out_specs, check_vma=False)
```

```python
import functools

import jax
import jax.numpy as jnp
from jax import lax
from jax.experimental import pallas as pl
from jax.experimental.pallas import tpu as pltpu
from jax.sharding import PartitionSpec as P


STEPS = 3
SHIFTS = (0.0, 1.0, 0.0)
WIDE = 32
LIMIT = 16 << 20
F32 = jnp.float32
BF16 = jnp.bfloat16

SMEM = pl.BlockSpec(memory_space=pltpu.SMEM)
VMEM = pl.BlockSpec(memory_space=pltpu.VMEM)
ANY = pl.BlockSpec(memory_space=pl.ANY)


def dot(a, b, contract):
    return lax.dot_general(a, b, (contract, ((), ())), preferred_element_type=F32)


def exact_dot(a, b, contract):
    return lax.dot_general(
        a, b, (contract, ((), ())), precision=lax.Precision.HIGHEST, preferred_element_type=F32
    )


def for_slots(slots, body):
    live = slots[0, slots.shape[1] - 1]

    def turns(size, first, count):
        def group(index, carry):
            entries = []
            for lane in range(size):
                code = slots[0, first + index * size + lane]
                entries.append((code & 255, (code >> 8) & 255, code >> 16))
            body(entries)
            return carry

        lax.fori_loop(0, count, group, 0)

    wide = (live + WIDE // 2 - 1) // WIDE
    left = live - wide * WIDE
    turns(WIDE, 0, wide)
    turns(WIDE // 2, wide * WIDE, (left > WIDE // 4).astype(jnp.int32))
    small = jnp.logical_and(left > 0, left <= WIDE // 4)
    turns(WIDE // 4, wide * WIDE, small.astype(jnp.int32))


def two_parts(values):
    high = values.astype(BF16).astype(F32)
    return jnp.concatenate([high, values - high], axis=0)


def add_products(entries, tiles, source, totals, forward):
    products = []
    for slot, row, col in entries:
        index = col if forward else row
        got = dot(source[index], tiles[slot], ((1,), (1,)) if forward else ((1,), (0,)))
        products.append(got if got.shape[0] == 8 else got[0:8] + got[8:16])
    for (slot, row, col), got in zip(entries, products):
        index = row if forward else col
        totals[index] = totals[index] + got


def fill_one_hot(index, table):
    width = table.shape[0]
    for begin in range(0, index.shape[1], width):
        low = index[:, begin : begin + width] & (width - 1)
        hit = lax.broadcasted_iota(jnp.int32, (width, width), 0) == low
        table[:, begin : begin + width] = jnp.where(hit, 1.0, 0.0).astype(BF16)


def list_slots(live, rows, cols, row_blocks, outputs):
    count = rows.shape[1]
    shape = (8, count)
    lane = lax.broadcasted_iota(jnp.int32, shape, 1)
    row_id = lax.broadcasted_iota(jnp.int32, shape, 0)
    row = jnp.broadcast_to(rows, shape)
    col = jnp.broadcast_to(cols, shape)
    outside = col >= row_blocks
    index = jnp.where(outside, by_side(col, row_blocks), col)
    fields = jnp.where(row_id == 0, lane, jnp.where(row_id == 1, row, index)).astype(F32)
    square = (count, count)
    first = lax.broadcasted_iota(jnp.int32, square, 0)
    second = lax.broadcasted_iota(jnp.int32, square, 1)
    before = jnp.where(first < second, 1.0, 0.0).astype(BF16)
    empty = (row_blocks << 8) | (row_blocks << 16)
    alive = lane < live
    outer = jnp.logical_and(alive, outside)
    side = index < row_blocks // 2
    masks = [
        jnp.logical_and(alive, jnp.logical_not(outside)),
        outer,
        jnp.logical_and(outer, side),
        jnp.logical_and(outer, jnp.logical_not(side)),
    ]
    ones = [jnp.where(mask, 1.0, 0.0) for mask in masks]
    ahead = dot(jnp.concatenate(ones, axis=0).astype(BF16), before, ((1,), (0,)))
    totals = [jnp.sum(one, axis=1, keepdims=True).astype(jnp.int32)[0:1] for one in ones]
    spots = [jnp.where(mask, ahead[8 * i : 8 * i + 8], -1.0)[0:1] for i, mask in enumerate(masks)]
    moved = [
        jnp.where(jnp.broadcast_to(spot, square).T == second.astype(F32), 1.0, 0.0).astype(BF16)
        for spot in spots
    ]
    placed = [dot(fields.astype(BF16), move, ((1,), (0,))).astype(jnp.int32) for move in moved]
    for out, total, place in zip(outputs, totals, placed):
        code = place[0:1] | (place[1:2] << 8) | (place[2:3] << 16)
        out[:, :count] = jnp.where(lane[0:1] < total, code, empty)
        out[:, count:] = jnp.where(lane[0:1] == count - 1, total, empty)


def index_kernel(
    row_blocks, counts, slot_rows, slot_cols, bound, warm,
    own, halo, near, far, table, high, hot, place, spread,
):
    list_slots(counts[0], slot_rows[...], slot_cols[...], row_blocks, (own, halo, near, far))
    even = lax.axis_index("rows") % 2 == 0
    upper = bound[1:2, :]
    lower = bound[0:1, :]
    index = jnp.concatenate(
        [jnp.where(even, upper, lower), jnp.where(even, lower, upper)], axis=1
    )
    main = hot.shape[1]
    width = table.shape[0]
    shift = width.bit_length() - 1
    rest = table.shape[1] - main
    high[...] = jnp.broadcast_to(index >> shift, high.shape)
    fill_one_hot(index, table)
    entry = lax.broadcasted_iota(jnp.int32, (8, rest), 1) + 1
    stacked = two_parts(entry.astype(F32))
    both = jnp.broadcast_to(index >> shift, (16, index.shape[1]))
    high_count = spread.shape[0] // 16
    for part in range(high_count):
        rows = slice(16 * part, 16 * part + 16)
        hot[rows, :] = jnp.where(both[:, :main] == part, 1.0, 0.0).astype(BF16)
        spread[rows, :] = jnp.where(both[:, main:] == part, stacked, 0.0).astype(BF16)
    got = dot(spread[...], table[:, main:], ((1,), (1,)))
    for part in range(high_count):
        one = got[16 * part : 16 * part + 8] + got[16 * part + 8 : 16 * part + 16]
        place[:, part * width : (part + 1) * width] = (one + 0.5).astype(jnp.int32) - 1


def gathered(code, sources):
    edge = code.shape[1]
    lane = code & (edge - 1)
    block = code >> (edge.bit_length() - 1)
    total = jnp.zeros(code.shape, F32)
    for index, source in enumerate(sources):
        moved = jnp.take_along_axis(source, lane, axis=1, mode="promise_in_bounds")
        total = jnp.where(block == index, moved, total)
    return total


def add_by_product(table, hot, spread, values, first):
    edge = values[0].shape[1]
    width = table.shape[0]
    count = len(values) * edge
    high_count = spread.shape[0] // 16
    for block, value in enumerate(values):
        for index in range(high_count):
            rows = slice(16 * index, 16 * index + 16)
            begin = first + block * edge
            spread[rows, block * edge : (block + 1) * edge] = hot[rows, begin : begin + edge] * value
    got = dot(spread[:, :count], table[:, first : first + count], ((1,), (1,)))
    result = []
    for index in range(high_count):
        one = got[16 * index : 16 * index + 8] + got[16 * index + 8 : 16 * index + 16]
        result += [one[:, begin : begin + edge] for begin in range(0, width, edge)]
    return result


def add_far(table, hot, place, spread, values):
    edge = values[0].shape[1]
    halo = table.shape[1] // 2
    count = (hot.shape[1] - halo) // edge
    result = add_by_product(table, hot, spread, values[:count], halo)
    last = [value.astype(F32) for value in values[count:]]
    last = [value[0:8] + value[8:16] for value in last]
    return [
        one + gathered(place[:, index * edge : (index + 1) * edge], last)
        for index, one in enumerate(result)
    ]


def pick_boundary(table, high, vector, scale, outs):
    width = table.shape[0]
    halo = table.shape[1] // 2
    high_count = vector.shape[1] // width
    rows = jnp.concatenate(
        [
            scale[:, index * width : (index + 1) * width]
            * vector[:, index * width : (index + 1) * width]
            for index in range(high_count)
        ],
        axis=0,
    ).astype(BF16)

    def picked(begin):
        cols = slice(begin, begin + width)
        got = dot(rows, table[:, cols], ((1,), (0,)))
        total = jnp.zeros((8, width), F32)
        for index in range(high_count):
            total = jnp.where(high[:, cols] == index, got[8 * index : 8 * index + 8], total)
        return total

    for side, out in enumerate(outs):
        for begin in range(0, halo // 2, width):
            first = picked(side * halo + begin)
            second = picked(side * halo + halo // 2 + begin)
            out[:, halo + begin : halo + begin + width] = jnp.concatenate(
                [first, second], axis=0
            ).astype(BF16)


def warm_kernel(out):
    out[...] = jnp.zeros_like(out)


def each_live(size, counts, block_rows, block_cols, spare_row, spare_col, body):
    live = counts[0]

    def group(index, carry):
        entries = []
        for lane in range(size):
            slot = index * size + lane
            dead = slot >= live
            entries.append(
                (
                    slot,
                    jnp.where(dead, spare_row, block_rows[slot]),
                    jnp.where(dead, spare_col, block_cols[slot]),
                )
            )
        return body(entries, carry)

    return lax.fori_loop(0, (live + size - 1) // size, group, (0, 0))


def by_side(col, row_blocks):
    even = 1 - lax.axis_index("rows") % 2
    return (col - row_blocks + even * (row_blocks // 2)) & (row_blocks - 1)


def setup_kernel(
    counts, block_rows, block_cols, tiles, high, first, second, inner, sums
):
    edge = tiles.shape[1]
    halo_blocks = first.shape[0]
    row_blocks = inner.shape[0]
    sums[...] = jnp.zeros_like(sums)

    def add(entries, carry):
        parts = [
            jnp.sum(tiles[slot].astype(F32).reshape(edge // 8, 8, edge), axis=0)
            for slot, row, col in entries
        ]
        for (slot, row, col), part in zip(entries, parts):
            inside = jnp.logical_or(col < row_blocks, col == sums.shape[0] - 1)
            index = jnp.where(inside, col, row_blocks + by_side(col, row_blocks))
            sums[index] = sums[index] + part
        return carry

    each_live(16, counts, block_rows, block_cols, row_blocks, sums.shape[0] - 1, add)
    for out, base in ((inner, 0), (first, row_blocks), (second, row_blocks + halo_blocks)):
        for index in range(out.shape[0]):
            out[index : index + 1, :] = jnp.sum(sums[base + index], axis=0, keepdims=True)


def degree_kernel(
    counts, block_rows, block_cols, tiles, inner, degree, row_sums
):
    edge = tiles.shape[1]
    row_blocks = inner.shape[0]
    row_sums[...] = jnp.zeros_like(row_sums)
    ones = jnp.ones((16, edge), BF16)

    def add(entries, carry):
        parts = [dot(ones, tiles[slot], ((1,), (1,)))[0:8] for slot, row, col in entries]
        for (slot, row, col), part in zip(entries, parts):
            row_sums[row] = row_sums[row] + part
        return carry

    each_live(WIDE, counts, block_rows, block_cols, row_blocks, 0, add)
    for index in range(row_blocks):
        degree[:, index * edge : (index + 1) * edge] = (
            1.0 + row_sums[index] + inner[index : index + 1, :]
        )


class Lists:
    def __init__(self, halo_in, halo, sem):
        self.halo = halo
        self.copies = [pltpu.make_async_copy(halo_in, halo, sem.at[0])]
        self.copies[0].start()

    def each(self, body):
        for copy in self.copies:
            copy.wait()
        self.copies = []
        for_slots(self.halo, body)


def send_products(lists, tiles, looks, vector, scale, source, sums, outs):
    edge = source.shape[2]
    row_blocks = source.shape[0] - 1
    half = row_blocks // 2
    for index in range(row_blocks):
        part = slice(index * edge, (index + 1) * edge)
        source[index] = two_parts(scale[:, part] * vector[:, part]).astype(BF16)
    source[row_blocks] = jnp.zeros_like(source[row_blocks])
    sums[...] = jnp.zeros_like(sums)
    lists.each(lambda entries: add_products(entries, tiles, source, sums, False))
    for side, out in enumerate(outs):
        for index in range(half):
            out[:, index * edge : (index + 1) * edge] = two_parts(
                sums[side * half + index]
            ).astype(BF16)
    pick_boundary(*looks, vector, scale, outs)


def first_kernel(
    halo_in, tiles, table, high, hot, place, degree, got_first, got_second, *rest
):
    starts = rest[:-9]
    out_first, out_second, vector, scale, source, spread, sums, halo, sem = rest[-9:]
    lists = Lists(halo_in, halo, sem)
    edge = tiles.shape[1]
    each = starts[0].shape[0]
    group = lax.axis_index("probe")
    for block in range(len(starts)):
        rows = starts[0][...]
        for other in range(1, len(starts)):
            rows = jnp.where(group == (block ^ other), starts[other][...], rows)
        vector[block * each : (block + 1) * each, :] = rows
    values = [
        two_parts(jnp.broadcast_to(got[i : i + 1, :], (8, edge))).astype(BF16)
        for got in (got_first, got_second)
        for i in range(got.shape[0])
    ]
    half = got_first.shape[0]
    near_parts = add_by_product(table, hot, spread, values[:half], 0)
    far_parts = add_far(table, hot, place, spread, values[half:])
    for index, part in enumerate(one + two for one, two in zip(near_parts, far_parts)):
        cols = slice(index * edge, (index + 1) * edge)
        total = degree[:, cols] + part
        root = lax.rsqrt(total)
        scale[:, cols] = root * (1.5 - 0.5 * total * root * root)
    send_products(
        lists, tiles, (table, high), vector, scale, source, sums, (out_first, out_second)
    )


def own_kernel(own, tiles, source, image, sums):
    edge = tiles.shape[1]
    sums[...] = jnp.zeros_like(sums)

    def add(entries):
        add_products(entries, tiles, source, sums, True)
        add_products(entries, tiles, source, sums, False)

    for_slots(own, add)
    for index in range(sums.shape[0] - 1):
        image[:, index * edge : (index + 1) * edge] = sums[index]


def unpack(got, side, halo, outside):
    edge = outside.shape[2]
    count = halo // edge
    values = []
    for index in range(count):
        half = index // (count // 2)
        begin = halo + (index % (count // 2)) * edge
        outside[side * count + index] = got[8 * half : 8 * half + 8, begin : begin + edge]
        values.append(got[:, index * edge : (index + 1) * edge])
    outside[2 * count] = jnp.zeros_like(outside[0])
    return values


def near_kernel(near, tiles, table, hot, image, got, total, spread, sums, outside):
    edge = tiles.shape[1]
    values = unpack(got, 0, table.shape[1] // 2, outside)
    for index, added in enumerate(add_by_product(table, hot, spread, values, 0)):
        sums[index] = added + image[:, index * edge : (index + 1) * edge]
    for_slots(near, lambda entries: add_products(entries, tiles, outside, sums, True))
    for index in range(sums.shape[0] - 1):
        total[:, index * edge : (index + 1) * edge] = sums[index]


def next_vector(
    shift, lists, tiles, looks, previous, scale, image, got, vector, spread, sums, outside
):
    edge = tiles.shape[1]
    values = unpack(got, 1, looks[0].shape[1] // 2, outside)
    for index, added in enumerate(add_far(*looks, spread, values)):
        sums[index] = added + image[:, index * edge : (index + 1) * edge]
    lists.each(lambda entries: add_products(entries, tiles, outside, sums, True))
    for index in range(sums.shape[0] - 1):
        part = slice(index * edge, (index + 1) * edge)
        old = previous[:, part]
        root = scale[:, part]
        vector[:, part] = root * (root * old) + root * sums[index] - shift * old


def middle_kernel(
    shift, far_in, halo_in, tiles, table, high, hot, place, previous, scale, image, got,
    out_first, out_second, vector, source,
    spread, sums, outside, far, far_sem, halo, halo_sem,
):
    far_list = Lists(far_in, far, far_sem)
    halo_list = Lists(halo_in, halo, halo_sem)
    next_vector(
        shift, far_list, tiles, (table, hot, place), previous, scale, image, got,
        vector, spread, sums, outside,
    )
    send_products(
        halo_list, tiles, (table, high), vector, scale, source, sums, (out_first, out_second)
    )


def three_parts(values):
    high = values.astype(BF16)
    rest = values - high.astype(F32)
    middle = rest.astype(BF16)
    return [high, middle, (rest - middle.astype(F32)).astype(BF16)]


def last_kernel(shift, far_in, tiles, table, hot, place, scale, image, got, *rest):
    vectors = rest[:STEPS]
    gram, vector, spread, sums, outside, far, sem = rest[STEPS:]
    lists = Lists(far_in, far, sem)
    next_vector(
        shift, lists, tiles, (table, hot, place), vectors[-1], scale, image, got,
        vector, spread, sums, outside,
    )
    basis = jnp.concatenate([one[...] for one in vectors] + [vector[...]], axis=0)
    size = basis.shape[0]
    parts = jnp.concatenate(three_parts(basis), axis=0)
    wide = dot(parts, parts, ((1,), (1,)))
    total = sum(
        wide[i * size : (i + 1) * size, j * size : (j + 1) * size]
        for i in reversed(range(3))
        for j in reversed(range(3))
    )
    packed = jnp.concatenate([total[8 * i : 8 * i + 8, :] for i in range(size // 8)], axis=1)
    for copy in range(gram.shape[0] // 8):
        gram[8 * copy : 8 * copy + 8, :] = packed


def final_kernel(node_total, grams, *rest):
    vectors = rest[: STEPS + 1]
    basis, alphas, betas = rest[STEPS + 1 :]
    size = 8 * (STEPS + 1)
    packed = grams[0:8, :]
    for copy in range(1, grams.shape[0] // 8):
        packed = packed + grams[8 * copy : 8 * copy + 8, :]
    packed = packed * (1.0 / node_total)
    gram = jnp.concatenate(
        [packed[:, i * size : (i + 1) * size] for i in range(STEPS + 1)], axis=0
    )
    row_ids = lax.broadcasted_iota(jnp.int32, (size, size), 0)
    col_ids = lax.broadcasted_iota(jnp.int32, (size, size), 1)
    unit = jnp.where(row_ids == col_ids, 1.0, 0.0)
    work = jnp.concatenate([gram, unit], axis=1)
    rows = lax.broadcasted_iota(jnp.int32, (size, 2 * size), 0)
    pivots = jnp.ones((size, 2 * size), F32)
    for begin in range(0, size, 8):
        columns = [
            jnp.broadcast_to(work[:, begin + c : begin + c + 1], (size, 2 * size)) for c in range(8)
        ]
        for c in range(8):
            k = begin + c
            pivot = columns[c][k : k + 1, :]
            pivots = jnp.where(rows == k, pivot, pivots)
            factor = jnp.where(rows > k, columns[c] * (1.0 / pivot), 0.0)
            work = work - factor * work[k : k + 1, :]
            for d in range(c + 1, 8):
                columns[d] = columns[d] - factor * columns[d][k : k + 1, :]
    work = work / jnp.sqrt(pivots)
    upper = jnp.where(row_ids <= col_ids, work[:, :size], 0.0)
    inverse = work[:, size:]
    own = jnp.where(row_ids // 8 == col_ids // 8, inverse, 0.0)
    moved = jnp.concatenate(
        [jnp.zeros((8, size), F32)]
        + [
            jnp.concatenate(
                [jnp.zeros((8, 8), F32), own[8 * i : 8 * i + 8, : size - 8]], axis=1
            )
            for i in range(STEPS)
        ],
        axis=0,
    )
    by_last = exact_dot(moved, upper, ((1,), (1,)))
    by_own = exact_dot(own, upper, ((1,), (1,)))
    small = unit[0:8, 0:8]

    def piece(table, i, j):
        return table[8 * i : 8 * i + 8, 8 * j : 8 * j + 8]

    for j in range(STEPS):
        beta = piece(by_last, j + 1, j + 1)
        alpha = (1.0 - SHIFTS[j]) * small - piece(by_last, j + 1, j)
        if j:
            alpha = alpha + exact_dot(piece(by_own, j, j - 1), piece(by_last, j, j), ((1,), (0,)))
        betas[j] = jnp.where(row_ids[0:8, 0:8] >= col_ids[0:8, 0:8], beta, 0.0)
        alphas[j] = alpha
    last = inverse[size - 8 :, :] * (-1.0) ** STEPS
    each = basis.shape[0]
    place = lax.axis_index("probe")
    ids = lax.broadcasted_iota(jnp.int32, (8, size), 0)
    chosen = jnp.zeros((8, size), F32)
    for index in range(each):
        line = jnp.sum(jnp.where(ids == place * each + index, last, 0.0), axis=0, keepdims=True)
        chosen = jnp.where(ids == index, line, chosen)
    total = exact_dot(chosen, jnp.concatenate([one[...] for one in vectors], axis=0), ((1,), (0,)))
    basis[...] = total[0:each]


def local(start_block, blocks, block_rows, block_cols, counts, boundary):
    each, rows_dev = start_block.shape
    slot_count, edge, _ = blocks.shape
    halo_width = boundary.shape[1]
    parts = lax.axis_size("rows")
    groups = lax.axis_size("probe")
    node_total = rows_dev * parts
    row_blocks = rows_dev // edge
    halo_blocks = halo_width // edge
    probes = each * groups
    width = 2 * edge
    shape = jax.ShapeDtypeStruct

    if parts % 2:
        raise ValueError("odd ring")
    matchings = (
        [(i, i ^ 1) for i in range(parts)],
        [(i, (i + 1) % parts if i % 2 else (i - 1) % parts) for i in range(parts)],
    )

    def exchange(first, second):
        got_second = lax.ppermute(second, "rows", matchings[1])
        got_first = lax.ppermute(first, "rows", matchings[0])
        return got_first, got_second

    listed = (1, 2 * slot_count)
    sums = pltpu.VMEM((row_blocks + 1, 8, edge), F32)
    outside = pltpu.VMEM((2 * halo_blocks + 1, 8, edge), BF16)
    fetched = [pltpu.SMEM(listed, jnp.int32), pltpu.SemaphoreType.DMA((1,))]

    def call(body, in_specs, out_shape, out_specs, scratch, flops=2 << 30):
        return pl.pallas_call(
            body,
            out_shape=out_shape,
            in_specs=in_specs,
            out_specs=out_specs,
            scratch_shapes=scratch,
            compiler_params=pltpu.CompilerParams(vmem_limit_bytes=LIMIT),
            cost_estimate=pl.CostEstimate(
                flops=flops, transcendentals=0, bytes_accessed=flops >> 11
            ),
        )

    starts = [start_block]
    for other in range(1, groups):
        pairs = [(i, i ^ other) for i in range(groups)]
        starts.append(lax.ppermute(start_block, "probe", pairs))
    warm = call(warm_kernel, [], shape((8, 128), F32), VMEM, [])()
    rest = halo_width // 2 // width * width
    main = 2 * halo_width - rest
    high_rows = 16 * (rows_dev // width)
    own, halo, near, far, table, high, hot, place = call(
        functools.partial(index_kernel, row_blocks),
        [SMEM, VMEM, VMEM, VMEM, ANY],
        (
            *(shape(listed, jnp.int32) for _ in range(4)),
            shape((width, 2 * halo_width), BF16),
            shape((8, 2 * halo_width), jnp.int32),
            shape((high_rows, main), BF16),
            shape((8, rows_dev), jnp.int32),
        ),
        (VMEM,) * 8,
        [pltpu.VMEM((high_rows, rest), BF16)],
        flops=1 << 20,
    )(counts, block_rows.reshape(1, -1), block_cols.reshape(1, -1), boundary, warm)
    low, up, inner = call(
        setup_kernel,
        [SMEM, SMEM, SMEM, VMEM, ANY],
        (
            shape((halo_blocks, edge), F32),
            shape((halo_blocks, edge), F32),
            shape((row_blocks, edge), F32),
        ),
        (VMEM,) * 3,
        [pltpu.VMEM((row_blocks + 2 * halo_blocks + 1, 8, edge), F32)],
    )(counts, block_rows, block_cols, blocks, high)
    got = exchange(low, up)
    spread = pltpu.VMEM((high_rows, halo_width), BF16)
    degree = call(
        degree_kernel, [SMEM, SMEM, SMEM, VMEM, VMEM], shape((8, rows_dev), F32), VMEM, [sums]
    )(counts, block_rows, block_cols, blocks, inner)

    message = shape((16, halo_width + halo_width // 2), BF16)
    vector_shape = shape((probes, rows_dev), F32)
    source_shape = shape((row_blocks + 1, 16, edge), BF16)
    first, second, vector, scale, source = call(
        first_kernel,
        [ANY] + [VMEM] * (8 + groups),
        (message, message, vector_shape, vector_shape, source_shape),
        (VMEM,) * 5,
        [spread, sums] + fetched,
    )(halo, blocks, table, high, hot, place, degree, *got, *starts)

    vectors = [vector]
    for step in range(STEPS):
        got = exchange(first, second)
        own_call = call(own_kernel, [SMEM, VMEM, VMEM], vector_shape, VMEM, [sums])
        image = own_call(own, blocks, source)
        image = call(
            near_kernel, [SMEM] + [VMEM] * 5, vector_shape, VMEM, [spread, sums, outside]
        )(near, blocks, table, hot, image, got[0])
        if step + 1 < STEPS:
            first, second, vector, source = call(
                functools.partial(middle_kernel, SHIFTS[step]),
                [ANY, ANY] + [VMEM] * 9,
                (message, message, vector_shape, source_shape),
                (VMEM,) * 4,
                [spread, sums, outside] + fetched + fetched,
            )(far, halo, blocks, table, high, hot, place, vectors[-1], scale, image, got[1])
        else:
            grams, vector = call(
                functools.partial(last_kernel, SHIFTS[step]),
                [ANY] + [VMEM] * (7 + STEPS),
                (shape((8 * parts, 128), F32), vector_shape),
                (VMEM,) * 2,
                [spread, sums, outside] + fetched,
            )(far, blocks, table, hot, place, scale, image, got[1], *vectors)
        vectors.append(vector)
    gathered = lax.all_to_all(grams, "rows", 0, 0, tiled=True)
    return call(
        functools.partial(final_kernel, float(node_total)),
        [VMEM] * (2 + STEPS),
        (
            shape((each, rows_dev), F32),
            shape((STEPS, probes, probes), F32),
            shape((STEPS, probes, probes), F32),
        ),
        (VMEM,) * 3,
        [],
    )(gathered, *vectors)


def solution(mesh):
    in_specs = (
        P("probe", "rows"),
        P("rows", None, None),
        P("rows"),
        P("rows"),
        P("rows"),
        P(None, "rows"),
    )
    out_specs = (P("probe", "rows"), P(), P())
    return jax.shard_map(local, mesh=mesh, in_specs=in_specs, out_specs=out_specs, check_vma=False)
```

```python
import functools

import jax
import jax.numpy as jnp
from jax import lax
from jax.experimental import pallas as pl
from jax.experimental.pallas import tpu as pltpu
from jax.sharding import PartitionSpec as P


STEPS = 3
SHIFTS = (0.0, 1.0, 0.0)
WIDE = 32
LIMIT = 16 << 20
F32 = jnp.float32
BF16 = jnp.bfloat16

SMEM = pl.BlockSpec(memory_space=pltpu.SMEM)
VMEM = pl.BlockSpec(memory_space=pltpu.VMEM)
ANY = pl.BlockSpec(memory_space=pl.ANY)


def dot(a, b, contract):
    return lax.dot_general(a, b, (contract, ((), ())), preferred_element_type=F32)


def exact_dot(a, b, contract):
    return lax.dot_general(
        a, b, (contract, ((), ())), precision=lax.Precision.HIGHEST, preferred_element_type=F32
    )


def for_slots(slots, body):
    live = slots[0, slots.shape[1] - 1]

    def turns(size, first, count):
        def group(index, carry):
            entries = []
            for lane in range(size):
                code = slots[0, first + index * size + lane]
                entries.append((code & 255, (code >> 8) & 255, code >> 16))
            body(entries)
            return carry

        lax.fori_loop(0, count, group, 0)

    wide = (live + WIDE // 2 - 1) // WIDE
    left = live - wide * WIDE
    turns(WIDE, 0, wide)
    turns(WIDE // 2, wide * WIDE, (left > WIDE // 4).astype(jnp.int32))
    small = jnp.logical_and(left > 0, left <= WIDE // 4)
    turns(WIDE // 4, wide * WIDE, small.astype(jnp.int32))


def two_parts(values):
    high = values.astype(BF16).astype(F32)
    return jnp.concatenate([high, values - high], axis=0)


def add_products(entries, tiles, source, totals, forward):
    products = []
    for slot, row, col in entries:
        index = col if forward else row
        got = dot(source[index], tiles[slot], ((1,), (1,)) if forward else ((1,), (0,)))
        products.append(got if got.shape[0] == 8 else got[0:8] + got[8:16])
    for (slot, row, col), got in zip(entries, products):
        index = row if forward else col
        totals[index] = totals[index] + got


def fill_one_hot(index, table):
    width = table.shape[0]
    for begin in range(0, index.shape[1], width):
        low = index[:, begin : begin + width] & (width - 1)
        hit = lax.broadcasted_iota(jnp.int32, (width, width), 0) == low
        table[:, begin : begin + width] = jnp.where(hit, 1.0, 0.0).astype(BF16)


def list_slots(live, rows, cols, row_blocks, outputs):
    count = rows.shape[1]
    shape = (8, count)
    lane = lax.broadcasted_iota(jnp.int32, shape, 1)
    row_id = lax.broadcasted_iota(jnp.int32, shape, 0)
    row = jnp.broadcast_to(rows, shape)
    col = jnp.broadcast_to(cols, shape)
    outside = col >= row_blocks
    index = jnp.where(outside, by_side(col, row_blocks), col)
    fields = jnp.where(row_id == 0, lane, jnp.where(row_id == 1, row, index)).astype(F32)
    square = (count, count)
    first = lax.broadcasted_iota(jnp.int32, square, 0)
    second = lax.broadcasted_iota(jnp.int32, square, 1)
    before = jnp.where(first < second, 1.0, 0.0).astype(BF16)
    empty = (row_blocks << 8) | (row_blocks << 16)
    alive = lane < live
    outer = jnp.logical_and(alive, outside)
    side = index < row_blocks // 2
    masks = [
        jnp.logical_and(alive, jnp.logical_not(outside)),
        outer,
        jnp.logical_and(outer, side),
        jnp.logical_and(outer, jnp.logical_not(side)),
    ]
    ones = [jnp.where(mask, 1.0, 0.0) for mask in masks]
    ahead = dot(jnp.concatenate(ones, axis=0).astype(BF16), before, ((1,), (0,)))
    totals = [jnp.sum(one, axis=1, keepdims=True).astype(jnp.int32)[0:1] for one in ones]
    spots = [jnp.where(mask, ahead[8 * i : 8 * i + 8], -1.0)[0:1] for i, mask in enumerate(masks)]
    moved = [
        jnp.where(jnp.broadcast_to(spot, square).T == second.astype(F32), 1.0, 0.0).astype(BF16)
        for spot in spots
    ]
    placed = [dot(fields.astype(BF16), move, ((1,), (0,))).astype(jnp.int32) for move in moved]
    for out, total, place in zip(outputs, totals, placed):
        code = place[0:1] | (place[1:2] << 8) | (place[2:3] << 16)
        out[:, :count] = jnp.where(lane[0:1] < total, code, empty)
        out[:, count:] = jnp.where(lane[0:1] == count - 1, total, empty)


def index_kernel(
    row_blocks, counts, slot_rows, slot_cols, bound, warm,
    own, halo, near, far, table, high, hot, place, spread,
):
    list_slots(counts[0], slot_rows[...], slot_cols[...], row_blocks, (own, halo, near, far))
    even = lax.axis_index("rows") % 2 == 0
    upper = bound[1:2, :]
    lower = bound[0:1, :]
    index = jnp.concatenate(
        [jnp.where(even, upper, lower), jnp.where(even, lower, upper)], axis=1
    )
    main = hot.shape[1]
    width = table.shape[0]
    shift = width.bit_length() - 1
    rest = table.shape[1] - main
    high[...] = jnp.broadcast_to(index >> shift, high.shape)
    fill_one_hot(index, table)
    entry = lax.broadcasted_iota(jnp.int32, (8, rest), 1) + 1
    stacked = two_parts(entry.astype(F32))
    both = jnp.broadcast_to(index >> shift, (16, index.shape[1]))
    high_count = spread.shape[0] // 16
    for part in range(high_count):
        rows = slice(16 * part, 16 * part + 16)
        hot[rows, :] = jnp.where(both[:, :main] == part, 1.0, 0.0).astype(BF16)
        spread[rows, :] = jnp.where(both[:, main:] == part, stacked, 0.0).astype(BF16)
    got = dot(spread[...], table[:, main:], ((1,), (1,)))
    for part in range(high_count):
        one = got[16 * part : 16 * part + 8] + got[16 * part + 8 : 16 * part + 16]
        place[:, part * width : (part + 1) * width] = (one + 0.5).astype(jnp.int32) - 1


def gathered(code, sources):
    edge = code.shape[1]
    lane = code & (edge - 1)
    block = code >> (edge.bit_length() - 1)
    total = jnp.zeros(code.shape, F32)
    for index, source in enumerate(sources):
        moved = jnp.take_along_axis(source, lane, axis=1, mode="promise_in_bounds")
        total = jnp.where(block == index, moved, total)
    return total


def add_by_product(table, hot, spread, values, first):
    edge = values[0].shape[1]
    width = table.shape[0]
    count = len(values) * edge
    high_count = spread.shape[0] // 16
    for block, value in enumerate(values):
        for index in range(high_count):
            rows = slice(16 * index, 16 * index + 16)
            begin = first + block * edge
            spread[rows, block * edge : (block + 1) * edge] = hot[rows, begin : begin + edge] * value
    got = dot(spread[:, :count], table[:, first : first + count], ((1,), (1,)))
    result = []
    for index in range(high_count):
        one = got[16 * index : 16 * index + 8] + got[16 * index + 8 : 16 * index + 16]
        result += [one[:, begin : begin + edge] for begin in range(0, width, edge)]
    return result


def add_far(table, hot, place, spread, values):
    edge = values[0].shape[1]
    halo = table.shape[1] // 2
    count = (hot.shape[1] - halo) // edge
    result = add_by_product(table, hot, spread, values[:count], halo)
    last = [value.astype(F32) for value in values[count:]]
    last = [value[0:8] + value[8:16] for value in last]
    return [
        one + gathered(place[:, index * edge : (index + 1) * edge], last)
        for index, one in enumerate(result)
    ]


def pick_boundary(table, high, vector, scale, outs):
    width = table.shape[0]
    halo = table.shape[1] // 2
    high_count = vector.shape[1] // width
    rows = jnp.concatenate(
        [
            scale[:, index * width : (index + 1) * width]
            * vector[:, index * width : (index + 1) * width]
            for index in range(high_count)
        ],
        axis=0,
    ).astype(BF16)

    def picked(begin):
        cols = slice(begin, begin + width)
        got = dot(rows, table[:, cols], ((1,), (0,)))
        total = jnp.zeros((8, width), F32)
        for index in range(high_count):
            total = jnp.where(high[:, cols] == index, got[8 * index : 8 * index + 8], total)
        return total

    for side, out in enumerate(outs):
        for begin in range(0, halo // 2, width):
            first = picked(side * halo + begin)
            second = picked(side * halo + halo // 2 + begin)
            out[:, halo + begin : halo + begin + width] = jnp.concatenate(
                [first, second], axis=0
            ).astype(BF16)


def warm_kernel(out):
    out[...] = jnp.zeros_like(out)


def each_live(size, counts, block_rows, block_cols, spare_row, spare_col, body):
    live = counts[0]

    def group(index, carry):
        entries = []
        for lane in range(size):
            slot = index * size + lane
            dead = slot >= live
            entries.append(
                (
                    slot,
                    jnp.where(dead, spare_row, block_rows[slot]),
                    jnp.where(dead, spare_col, block_cols[slot]),
                )
            )
        return body(entries, carry)

    return lax.fori_loop(0, (live + size - 1) // size, group, (0, 0))


def by_side(col, row_blocks):
    even = 1 - lax.axis_index("rows") % 2
    return (col - row_blocks + even * (row_blocks // 2)) & (row_blocks - 1)


def setup_kernel(
    counts, block_rows, block_cols, tiles, high, first, second, inner, sums
):
    edge = tiles.shape[1]
    halo_blocks = first.shape[0]
    row_blocks = inner.shape[0]
    sums[...] = jnp.zeros_like(sums)

    def add(entries, carry):
        parts = [
            jnp.sum(tiles[slot].astype(F32).reshape(edge // 8, 8, edge), axis=0)
            for slot, row, col in entries
        ]
        for (slot, row, col), part in zip(entries, parts):
            inside = jnp.logical_or(col < row_blocks, col == sums.shape[0] - 1)
            index = jnp.where(inside, col, row_blocks + by_side(col, row_blocks))
            sums[index] = sums[index] + part
        return carry

    each_live(16, counts, block_rows, block_cols, row_blocks, sums.shape[0] - 1, add)
    for out, base in ((inner, 0), (first, row_blocks), (second, row_blocks + halo_blocks)):
        for index in range(out.shape[0]):
            out[index : index + 1, :] = jnp.sum(sums[base + index], axis=0, keepdims=True)


def degree_kernel(
    counts, block_rows, block_cols, tiles, inner, degree, row_sums
):
    edge = tiles.shape[1]
    row_blocks = inner.shape[0]
    row_sums[...] = jnp.zeros_like(row_sums)
    ones = jnp.ones((16, edge), BF16)

    def add(entries, carry):
        parts = [dot(ones, tiles[slot], ((1,), (1,)))[0:8] for slot, row, col in entries]
        for (slot, row, col), part in zip(entries, parts):
            row_sums[row] = row_sums[row] + part
        return carry

    each_live(WIDE, counts, block_rows, block_cols, row_blocks, 0, add)
    for index in range(row_blocks):
        degree[:, index * edge : (index + 1) * edge] = (
            1.0 + row_sums[index] + inner[index : index + 1, :]
        )


class Lists:
    def __init__(self, halo_in, halo, sem):
        self.halo = halo
        self.copies = [pltpu.make_async_copy(halo_in, halo, sem.at[0])]
        self.copies[0].start()

    def each(self, body):
        for copy in self.copies:
            copy.wait()
        self.copies = []
        for_slots(self.halo, body)


def send_products(lists, tiles, looks, vector, scale, source, sums, outs):
    edge = source.shape[2]
    row_blocks = source.shape[0] - 1
    half = row_blocks // 2
    for index in range(row_blocks):
        part = slice(index * edge, (index + 1) * edge)
        source[index] = two_parts(scale[:, part] * vector[:, part]).astype(BF16)
    source[row_blocks] = jnp.zeros_like(source[row_blocks])
    sums[...] = jnp.zeros_like(sums)
    lists.each(lambda entries: add_products(entries, tiles, source, sums, False))
    for side, out in enumerate(outs):
        for index in range(half):
            out[:, index * edge : (index + 1) * edge] = two_parts(
                sums[side * half + index]
            ).astype(BF16)
    pick_boundary(*looks, vector, scale, outs)


def first_kernel(
    halo_in, tiles, table, high, hot, place, degree, got_first, got_second, *rest
):
    starts = rest[:-9]
    out_first, out_second, vector, scale, source, spread, sums, halo, sem = rest[-9:]
    lists = Lists(halo_in, halo, sem)
    edge = tiles.shape[1]
    each = starts[0].shape[0]
    group = lax.axis_index("probe")
    for block in range(len(starts)):
        rows = starts[0][...]
        for other in range(1, len(starts)):
            rows = jnp.where(group == (block ^ other), starts[other][...], rows)
        vector[block * each : (block + 1) * each, :] = rows
    values = [
        two_parts(jnp.broadcast_to(got[i : i + 1, :], (8, edge))).astype(BF16)
        for got in (got_first, got_second)
        for i in range(got.shape[0])
    ]
    half = got_first.shape[0]
    near_parts = add_by_product(table, hot, spread, values[:half], 0)
    far_parts = add_far(table, hot, place, spread, values[half:])
    for index, part in enumerate(one + two for one, two in zip(near_parts, far_parts)):
        cols = slice(index * edge, (index + 1) * edge)
        total = degree[:, cols] + part
        root = lax.rsqrt(total)
        scale[:, cols] = root * (1.5 - 0.5 * total * root * root)
    send_products(
        lists, tiles, (table, high), vector, scale, source, sums, (out_first, out_second)
    )


def own_kernel(own, tiles, source, image, sums):
    edge = tiles.shape[1]
    sums[...] = jnp.zeros_like(sums)

    def add(entries):
        add_products(entries, tiles, source, sums, True)
        add_products(entries, tiles, source, sums, False)

    for_slots(own, add)
    for index in range(sums.shape[0] - 1):
        image[:, index * edge : (index + 1) * edge] = sums[index]


def unpack(got, side, halo, outside):
    edge = outside.shape[2]
    count = halo // edge
    values = []
    for index in range(count):
        half = index // (count // 2)
        begin = halo + (index % (count // 2)) * edge
        outside[side * count + index] = got[8 * half : 8 * half + 8, begin : begin + edge]
        values.append(got[:, index * edge : (index + 1) * edge])
    outside[2 * count] = jnp.zeros_like(outside[0])
    return values


def near_kernel(near_in, tiles, table, hot, image, got, total, spread, sums, outside, near, sem):
    lists = Lists(near_in, near, sem)
    edge = tiles.shape[1]
    values = unpack(got, 0, table.shape[1] // 2, outside)
    for index, added in enumerate(add_by_product(table, hot, spread, values, 0)):
        sums[index] = added + image[:, index * edge : (index + 1) * edge]
    lists.each(lambda entries: add_products(entries, tiles, outside, sums, True))
    for index in range(sums.shape[0] - 1):
        total[:, index * edge : (index + 1) * edge] = sums[index]


def next_vector(
    shift, lists, tiles, looks, previous, scale, image, got, vector, spread, sums, outside
):
    edge = tiles.shape[1]
    values = unpack(got, 1, looks[0].shape[1] // 2, outside)
    for index, added in enumerate(add_far(*looks, spread, values)):
        sums[index] = added + image[:, index * edge : (index + 1) * edge]
    lists.each(lambda entries: add_products(entries, tiles, outside, sums, True))
    for index in range(sums.shape[0] - 1):
        part = slice(index * edge, (index + 1) * edge)
        old = previous[:, part]
        root = scale[:, part]
        vector[:, part] = root * (root * old) + root * sums[index] - shift * old


def middle_kernel(
    shift, far_in, halo_in, tiles, table, high, hot, place, previous, scale, image, got,
    out_first, out_second, vector, source,
    spread, sums, outside, far, far_sem, halo, halo_sem,
):
    far_list = Lists(far_in, far, far_sem)
    halo_list = Lists(halo_in, halo, halo_sem)
    next_vector(
        shift, far_list, tiles, (table, hot, place), previous, scale, image, got,
        vector, spread, sums, outside,
    )
    send_products(
        halo_list, tiles, (table, high), vector, scale, source, sums, (out_first, out_second)
    )


def three_parts(values):
    high = values.astype(BF16)
    rest = values - high.astype(F32)
    middle = rest.astype(BF16)
    return [high, middle, (rest - middle.astype(F32)).astype(BF16)]


def last_kernel(shift, far_in, tiles, table, hot, place, scale, image, got, *rest):
    vectors = rest[:STEPS]
    gram, vector, spread, sums, outside, far, sem = rest[STEPS:]
    lists = Lists(far_in, far, sem)
    next_vector(
        shift, lists, tiles, (table, hot, place), vectors[-1], scale, image, got,
        vector, spread, sums, outside,
    )
    basis = jnp.concatenate([one[...] for one in vectors] + [vector[...]], axis=0)
    size = basis.shape[0]
    parts = jnp.concatenate(three_parts(basis), axis=0)
    wide = dot(parts, parts, ((1,), (1,)))
    total = sum(
        wide[i * size : (i + 1) * size, j * size : (j + 1) * size]
        for i in reversed(range(3))
        for j in reversed(range(3))
    )
    packed = jnp.concatenate([total[8 * i : 8 * i + 8, :] for i in range(size // 8)], axis=1)
    for copy in range(gram.shape[0] // 8):
        gram[8 * copy : 8 * copy + 8, :] = packed


def final_kernel(node_total, grams, *rest):
    vectors = rest[: STEPS + 1]
    basis, alphas, betas = rest[STEPS + 1 :]
    size = 8 * (STEPS + 1)
    packed = grams[0:8, :]
    for copy in range(1, grams.shape[0] // 8):
        packed = packed + grams[8 * copy : 8 * copy + 8, :]
    packed = packed * (1.0 / node_total)
    gram = jnp.concatenate(
        [packed[:, i * size : (i + 1) * size] for i in range(STEPS + 1)], axis=0
    )
    row_ids = lax.broadcasted_iota(jnp.int32, (size, size), 0)
    col_ids = lax.broadcasted_iota(jnp.int32, (size, size), 1)
    unit = jnp.where(row_ids == col_ids, 1.0, 0.0)
    work = jnp.concatenate([gram, unit], axis=1)
    rows = lax.broadcasted_iota(jnp.int32, (size, 2 * size), 0)
    pivots = jnp.ones((size, 2 * size), F32)
    for begin in range(0, size, 8):
        columns = [
            jnp.broadcast_to(work[:, begin + c : begin + c + 1], (size, 2 * size)) for c in range(8)
        ]
        for c in range(8):
            k = begin + c
            pivot = columns[c][k : k + 1, :]
            pivots = jnp.where(rows == k, pivot, pivots)
            factor = jnp.where(rows > k, columns[c] * (1.0 / pivot), 0.0)
            work = work - factor * work[k : k + 1, :]
            for d in range(c + 1, 8):
                columns[d] = columns[d] - factor * columns[d][k : k + 1, :]
    work = work / jnp.sqrt(pivots)
    upper = jnp.where(row_ids <= col_ids, work[:, :size], 0.0)
    inverse = work[:, size:]
    own = jnp.where(row_ids // 8 == col_ids // 8, inverse, 0.0)
    moved = jnp.concatenate(
        [jnp.zeros((8, size), F32)]
        + [
            jnp.concatenate(
                [jnp.zeros((8, 8), F32), own[8 * i : 8 * i + 8, : size - 8]], axis=1
            )
            for i in range(STEPS)
        ],
        axis=0,
    )
    by_last = exact_dot(moved, upper, ((1,), (1,)))
    by_own = exact_dot(own, upper, ((1,), (1,)))
    small = unit[0:8, 0:8]

    def piece(table, i, j):
        return table[8 * i : 8 * i + 8, 8 * j : 8 * j + 8]

    for j in range(STEPS):
        beta = piece(by_last, j + 1, j + 1)
        alpha = (1.0 - SHIFTS[j]) * small - piece(by_last, j + 1, j)
        if j:
            alpha = alpha + exact_dot(piece(by_own, j, j - 1), piece(by_last, j, j), ((1,), (0,)))
        betas[j] = jnp.where(row_ids[0:8, 0:8] >= col_ids[0:8, 0:8], beta, 0.0)
        alphas[j] = alpha
    last = inverse[size - 8 :, :] * (-1.0) ** STEPS
    each = basis.shape[0]
    place = lax.axis_index("probe")
    ids = lax.broadcasted_iota(jnp.int32, (8, size), 0)
    chosen = jnp.zeros((8, size), F32)
    for index in range(each):
        line = jnp.sum(jnp.where(ids == place * each + index, last, 0.0), axis=0, keepdims=True)
        chosen = jnp.where(ids == index, line, chosen)
    total = exact_dot(chosen, jnp.concatenate([one[...] for one in vectors], axis=0), ((1,), (0,)))
    basis[...] = total[0:each]


def local(start_block, blocks, block_rows, block_cols, counts, boundary):
    each, rows_dev = start_block.shape
    slot_count, edge, _ = blocks.shape
    halo_width = boundary.shape[1]
    parts = lax.axis_size("rows")
    groups = lax.axis_size("probe")
    node_total = rows_dev * parts
    row_blocks = rows_dev // edge
    halo_blocks = halo_width // edge
    probes = each * groups
    width = 2 * edge
    shape = jax.ShapeDtypeStruct

    if parts % 2:
        raise ValueError("odd ring")
    matchings = (
        [(i, i ^ 1) for i in range(parts)],
        [(i, (i + 1) % parts if i % 2 else (i - 1) % parts) for i in range(parts)],
    )

    def exchange(first, second):
        got_second = lax.ppermute(second, "rows", matchings[1])
        got_first = lax.ppermute(first, "rows", matchings[0])
        return got_first, got_second

    listed = (1, 2 * slot_count)
    sums = pltpu.VMEM((row_blocks + 1, 8, edge), F32)
    outside = pltpu.VMEM((2 * halo_blocks + 1, 8, edge), BF16)
    fetched = [pltpu.SMEM(listed, jnp.int32), pltpu.SemaphoreType.DMA((1,))]

    def call(body, in_specs, out_shape, out_specs, scratch, flops=2 << 30):
        return pl.pallas_call(
            body,
            out_shape=out_shape,
            in_specs=in_specs,
            out_specs=out_specs,
            scratch_shapes=scratch,
            compiler_params=pltpu.CompilerParams(vmem_limit_bytes=LIMIT),
            cost_estimate=pl.CostEstimate(
                flops=flops, transcendentals=0, bytes_accessed=flops >> 11
            ),
        )

    starts = [start_block]
    for other in range(1, groups):
        pairs = [(i, i ^ other) for i in range(groups)]
        starts.append(lax.ppermute(start_block, "probe", pairs))
    warm = call(warm_kernel, [], shape((8, 128), F32), VMEM, [])()
    rest = halo_width // 2 // width * width
    main = 2 * halo_width - rest
    high_rows = 16 * (rows_dev // width)
    own, halo, near, far, table, high, hot, place = call(
        functools.partial(index_kernel, row_blocks),
        [SMEM, VMEM, VMEM, VMEM, ANY],
        (
            *(shape(listed, jnp.int32) for _ in range(4)),
            shape((width, 2 * halo_width), BF16),
            shape((8, 2 * halo_width), jnp.int32),
            shape((high_rows, main), BF16),
            shape((8, rows_dev), jnp.int32),
        ),
        (VMEM,) * 8,
        [pltpu.VMEM((high_rows, rest), BF16)],
        flops=1 << 20,
    )(counts, block_rows.reshape(1, -1), block_cols.reshape(1, -1), boundary, warm)
    low, up, inner = call(
        setup_kernel,
        [SMEM, SMEM, SMEM, VMEM, ANY],
        (
            shape((halo_blocks, edge), F32),
            shape((halo_blocks, edge), F32),
            shape((row_blocks, edge), F32),
        ),
        (VMEM,) * 3,
        [pltpu.VMEM((row_blocks + 2 * halo_blocks + 1, 8, edge), F32)],
    )(counts, block_rows, block_cols, blocks, high)
    got = exchange(low, up)
    spread = pltpu.VMEM((high_rows, halo_width), BF16)
    degree = call(
        degree_kernel, [SMEM, SMEM, SMEM, VMEM, VMEM], shape((8, rows_dev), F32), VMEM, [sums]
    )(counts, block_rows, block_cols, blocks, inner)

    message = shape((16, halo_width + halo_width // 2), BF16)
    vector_shape = shape((probes, rows_dev), F32)
    source_shape = shape((row_blocks + 1, 16, edge), BF16)
    first, second, vector, scale, source = call(
        first_kernel,
        [ANY] + [VMEM] * (8 + groups),
        (message, message, vector_shape, vector_shape, source_shape),
        (VMEM,) * 5,
        [spread, sums] + fetched,
    )(halo, blocks, table, high, hot, place, degree, *got, *starts)

    vectors = [vector]
    for step in range(STEPS):
        got = exchange(first, second)
        own_call = call(own_kernel, [SMEM, VMEM, VMEM], vector_shape, VMEM, [sums])
        image = own_call(own, blocks, source)
        image = call(
            near_kernel, [ANY] + [VMEM] * 5, vector_shape, VMEM, [spread, sums, outside] + fetched
        )(near, blocks, table, hot, image, got[0])
        if step + 1 < STEPS:
            first, second, vector, source = call(
                functools.partial(middle_kernel, SHIFTS[step]),
                [ANY, ANY] + [VMEM] * 9,
                (message, message, vector_shape, source_shape),
                (VMEM,) * 4,
                [spread, sums, outside] + fetched + fetched,
            )(far, halo, blocks, table, high, hot, place, vectors[-1], scale, image, got[1])
        else:
            grams, vector = call(
                functools.partial(last_kernel, SHIFTS[step]),
                [ANY] + [VMEM] * (7 + STEPS),
                (shape((8 * parts, 128), F32), vector_shape),
                (VMEM,) * 2,
                [spread, sums, outside] + fetched,
            )(far, blocks, table, hot, place, scale, image, got[1], *vectors)
        vectors.append(vector)
    gathered = lax.all_to_all(grams, "rows", 0, 0, tiled=True)
    return call(
        functools.partial(final_kernel, float(node_total)),
        [VMEM] * (2 + STEPS),
        (
            shape((each, rows_dev), F32),
            shape((STEPS, probes, probes), F32),
            shape((STEPS, probes, probes), F32),
        ),
        (VMEM,) * 3,
        [],
    )(gathered, *vectors)


def solution(mesh):
    in_specs = (
        P("probe", "rows"),
        P("rows", None, None),
        P("rows"),
        P("rows"),
        P("rows"),
        P(None, "rows"),
    )
    out_specs = (P("probe", "rows"), P(), P())
    return jax.shard_map(local, mesh=mesh, in_specs=in_specs, out_specs=out_specs, check_vma=False)
```
